32 devices in a mesh: chain: 8 (over y, x, core), col: 4 (over z).
Axes of the slice: x: 2, y: 2, z: 4, core: 2. Of those that a mesh axis runs over, the one named last changes fastest.
Arguments:
- rhs: bfloat16 [16, 64, 2560], P('chain', None, 'col'), may hold values from -6 to 6
- block_inverse: bfloat16 [16, 2560, 2560], P('chain', 'col'), as said below
- entry_factor: bfloat16 [16, 2560, 128], P('chain', 'col'), as said below
- exit_factor: bfloat16 [16, 2560, 128], P('chain', 'col'), as said below
- previous: bfloat16 [64, 2560], P(None, 'col'), may hold values from -6 to 6
Outputs:
- solution: float32 [16, 64, 2560], P('chain', None, 'col')
The draws below stay inside these ranges and needn't reach their ends.
Inputs may be any that keep to these rules, and one draw needn't show every extreme that they name: Every block of block_inverse equals its own transpose. `entry_factor`: entries are independent, of mean zero. `exit_factor`: entries are independent, of mean zero.
All inputs are finite; a program needn't handle non-finite values.
Results may differ from the reference program's by a relative error of at most 0.0003.
Values may be sent and summed in bfloat16 or wider, within the bound.
A program may use at most 64 MiB of HBM per device.

```python
import jax
import jax.numpy as jnp
from jax import lax

B = 2560
NX = 128
COLS = 64
INTERVALS = 16


def draw_block_inverse(key, part):

    def draw_block(interval):
        subkey = jax.random.fold_in(key, interval)
        first_key, second_key = jax.random.split(subkey)
        random_part = jax.random.normal(first_key, (B, B), jnp.float32)
        symmetric = (random_part + random_part.T) * (0.6 / (2.0 * B) ** 0.5)
        diagonal_part = jax.random.uniform(second_key, (B,), jnp.float32, 0.5, 2.0)
        return (symmetric + jnp.diag(diagonal_part)).astype(jnp.bfloat16)
    return lax.map(draw_block, jnp.arange(INTERVALS))


def draw_factor(key, spread):
    shape = (INTERVALS, B, NX)
    values = jax.random.truncated_normal(key, -3.0, 3.0, shape, jnp.float32) * (spread / 0.9866)
    return values.astype(jnp.bfloat16)


def draw_entry_factor(key, part):
    return draw_factor(jax.random.fold_in(key, 11), (NX * 5.0 / 4.0) ** (-0.5))


def draw_exit_factor(key, part):
    return draw_factor(jax.random.fold_in(key, 23), (1.0 * B) ** (-0.5))


def block_scale(rng, extent, cuts, low, high):
    def one(position, parts):
        draws = jax.random.uniform(jax.random.fold_in(jax.random.fold_in(rng, 6), position), (parts,), jnp.float32, low / len(cuts), high / len(cuts))
        return jnp.repeat(jnp.exp(draws), extent[position] // parts).reshape((-1,) + (1,) * (len(extent) - position - 1))

    factor_of = one(*cuts[0])
    for cut in cuts[1:]:
        factor_of = factor_of * one(*cut)
    return factor_of


def bell_draw(key, shape, scale, reach, cuts=(), dtype=jnp.bfloat16):
    result = scale * jax.random.normal(key, shape, jnp.float32)
    if cuts:
        result = result * block_scale(key, shape, cuts, -0.22, 0.18)
    return jnp.clip(result, -reach, reach).astype(dtype)


def setup_inputs(seed: int = 0) -> dict:
    streams_of = jax.random.split(jax.random.key(seed), 6)
    rhs = bell_draw(streams_of[0], (INTERVALS, COLS, B), 1.0, 6.0, ((0, 8), (2, 4)))
    block_inverse = draw_block_inverse(jax.random.fold_in(streams_of[5], 71), 0)
    entry_factor = draw_entry_factor(jax.random.fold_in(streams_of[5], 71), 0)
    exit_factor = draw_exit_factor(jax.random.fold_in(streams_of[5], 71), 0)
    previous = bell_draw(streams_of[4], (COLS, B), 1.0, 6.0, ((1, 4),))
    return {"rhs": rhs, "block_inverse": block_inverse, "entry_factor": entry_factor, "exit_factor": exit_factor, "previous": previous}


def reference(rhs, block_inverse, entry_factor, exit_factor, previous):
    exact = lax.Precision.HIGHEST
    total_intervals = rhs.shape[0]
    carry_state = jnp.dot(previous, exit_factor[0], preferred_element_type=jnp.float32)
    applied_list = []
    couplings = []
    for interval in range(total_intervals):
        solved = rhs[interval].astype(jnp.float32) - jnp.dot(carry_state, entry_factor[interval].astype(jnp.float32).T, precision=exact)
        solved_low = solved.astype(jnp.bfloat16)
        applied_list.append(jnp.dot(solved_low, block_inverse[interval], preferred_element_type=jnp.float32))
        if interval + 1 < total_intervals:
            following = exit_factor[interval + 1]
            couple = -jnp.dot(entry_factor[interval].T, following, preferred_element_type=jnp.float32)
            source = jnp.dot(rhs[interval], following, preferred_element_type=jnp.float32)
            carry_state = jnp.dot(carry_state, couple, precision=exact) + source
            couplings.append(couple)
    behind = jnp.zeros((rhs.shape[1], entry_factor.shape[2]), jnp.float32)
    results = [None] * total_intervals
    for interval in reversed(range(total_intervals)):
        applied = applied_list[interval]
        if interval + 1 < total_intervals:
            results[interval] = applied - jnp.dot(behind, exit_factor[interval + 1].astype(jnp.float32).T, precision=exact)
        else:
            results[interval] = applied
        if interval > 0:
            carried = jnp.dot(applied.astype(jnp.bfloat16), entry_factor[interval], preferred_element_type=jnp.float32)
            if interval + 1 < total_intervals:
                behind = jnp.dot(behind, couplings[interval].T, precision=exact) + carried
            else:
                behind = carried
    return jnp.stack(results)
```

```python
import functools

import jax
import jax.numpy as jnp
from jax import lax
from jax.experimental import pallas as pl
from jax.experimental.pallas import tpu as pltpu
from jax.sharding import PartitionSpec as P

MESH = pl.DeviceIdType.MESH
F32 = jnp.float32
BF16 = jnp.bfloat16


def dot_t(a, b):
    return lax.dot_general(a, b, (((1,), (1,)), ((), ())), preferred_element_type=F32)


def terms(x):
    first = x.astype(BF16)
    rest = x - first.astype(F32)
    second = rest.astype(BF16)
    third = (rest - second.astype(F32)).astype(BF16)
    return first, second, third


def split_dot_t(x, low):
    rows = x.shape[0]
    product = dot_t(jnp.concatenate(terms(x), axis=0), low)
    return (product[2 * rows:] + product[rows:2 * rows]) + product[:rows]


def wide(parts):
    a1, a2, a3 = parts
    return jnp.concatenate([a3, a2, a1, a2, a1, a1], axis=1)


def tall(parts, axis):
    b1, b2, b3 = parts
    return jnp.concatenate([b1, b2, b3, b1, b2, b1], axis=axis)


def exact_dot(a, b):
    return jnp.dot(wide(terms(a)), tall(terms(b), 0), preferred_element_type=F32)


def exact_dot_t(a, b):
    return dot_t(wide(terms(a)), tall(terms(b), 1))


def kernel(
    n, m, rhs_hbm, binv_hbm, entry_hbm, exit_hbm, prev_hbm, out_ref,
    rhs, binv, entry, exits, prev, arriving,
    parts, parts_in, opening, opening_in, sums, prefix, prefix_add, ahead, after,
    comp, gathered, states_out, states, forward, applied, carried, carried_in,
    carried_sum, back, back_in, local, behind_out, behind,
    local_sem, exit_sem, part_send, part_recv, sum_send, sum_recv, open_send, open_recv,
    comp_send, comp_recv, state_send, state_recv, fwd_send, fwd_recv,
    car_send, car_recv, back_send, back_recv, beh_send, beh_recv,
):
    c = lax.axis_index("chain")
    k = lax.axis_index("col")
    count, columns, width = rhs.shape
    nx = entry.shape[2]
    half = columns // 2
    window = nx + half
    chips = n // 2
    q = c // 2
    core = lax.rem(c, 2)
    mids = (m // 2 - 1, m // 2)
    blocks = 2 * count
    h = jnp.clip(k - mids[0], 0, 1)
    is_hub = (core == 1) & (k >= mids[0]) & (k <= mids[1])
    unsent = []

    def hub(side):
        return {"chain": 2 * q + 1, "col": mids[0] + side}

    def is_side(side):
        return (core == 1) & (k == mids[side])

    def remote(src, dst, send, recv, where):
        return pltpu.make_async_remote_copy(
            src_ref=src, dst_ref=dst, send_sem=send, recv_sem=recv,
            device_id=where, device_id_type=MESH,
        )

    def send(condition, *args):
        @pl.when(condition)
        def _():
            remote(*args).start()

        unsent.append((condition, args))

    here = {"chain": c, "col": k}
    loads = [
        pltpu.make_async_copy(exit_hbm, exits, local_sem.at[0]),
        pltpu.make_async_copy(entry_hbm, entry, local_sem.at[1]),
        pltpu.make_async_copy(rhs_hbm, rhs, local_sem.at[2]),
        pltpu.make_async_copy(prev_hbm, prev, local_sem.at[3]),
    ] + [
        pltpu.make_async_copy(binv_hbm.at[p], binv.at[p], local_sem.at[4 + p])
        for p in range(count)
    ]
    for load in loads:
        load.start()

    barrier = pltpu.get_barrier_semaphore()
    for d in range(1, m):
        for other in range(2):
            pl.semaphore_signal(
                barrier, 1, device_id={"chain": 2 * q + other, "col": lax.rem(k + d, m)},
                device_id_type=MESH,
            )
    pl.semaphore_signal(barrier, 1, device_id={"chain": 2 * q + 1 - core}, device_id_type=MESH)

    beside = c + 2 * core - 1
    has_beside = (beside >= 0) & (beside < n)

    @pl.when(has_beside)
    def _():
        pl.semaphore_signal(barrier, 1, device_id={"chain": beside}, device_id_type=MESH)

    @pl.when(is_hub)
    def _():
        for d in range(1, chips):
            pl.semaphore_signal(
                barrier, 1, device_id={"chain": 2 * lax.rem(q + d, chips) + 1},
                device_id_type=MESH,
            )

    @pl.when(c == n - 1)
    def _():
        arriving[...] = jnp.zeros_like(arriving)

    for load in loads[:4]:
        load.wait()

    @pl.when(c == 0)
    def _():
        opening[...] = jnp.dot(prev[...], exits[0], preferred_element_type=F32)

    def following(p):
        return exits[p + 1] if p + 1 < count else arriving[...]

    def part(p):
        after_p = following(p)
        source = jnp.dot(rhs[p], after_p, preferred_element_type=F32)
        parts[p, :half] = source[:half]
        parts[p, half:window] = -lax.dot_general(
            entry[p], after_p, (((0,), (0,)), ((), ())), preferred_element_type=F32
        )
        parts[p, window:] = source[half:]

    for p in range(count - 1):
        part(p)

    expected = 2 * m - 1 + jnp.where(has_beside, 1, 0) + jnp.where(is_hub, chips - 1, 0)
    pl.semaphore_wait(barrier, expected)

    send(c > 0, exits.at[0], arriving, exit_sem.at[0], exit_sem.at[1], {"chain": c - 1})
    for side in range(2):
        send(
            c == 0, opening.at[pl.ds(side * half, half)], opening_in.at[k],
            open_send.at[side], open_recv.at[k], hub(side),
        )

    def early_owner(j):
        return 0 if j < count else 1

    for p in range(count):
        if p + 1 == count:
            @pl.when(c < n - 1)
            def _():
                remote(
                    exits.at[0], arriving, exit_sem.at[0], exit_sem.at[1], here
                ).wait_recv()
            part(p)
        send(
            core == 0, parts.at[p], parts_in.at[0, k, p],
            part_send.at[p, 0], part_recv.at[0, k, p], hub(0),
        )
        if p + 1 < count:
            send(
                (core == 1) & jnp.logical_not(is_side(1)), parts.at[p], parts_in.at[1, k, p],
                part_send.at[p, 1], part_recv.at[1, k, p], hub(1),
            )
        else:
            for side in range(2):
                rows = pl.ds(side * half, window)
                send(
                    (core == 1) & jnp.logical_not(is_side(side)), parts.at[p, rows],
                    parts_in.at[1, k, p, rows], part_send.at[p, side],
                    part_recv.at[1, k, p], hub(side),
                )

    mine = pl.ds(pl.multiple_of(h * half, 8), window)
    yours = pl.ds(pl.multiple_of((1 - h) * half, 8), window)
    source_rows = pl.ds(pl.multiple_of(h * window, 8), half)

    def coupling(j):
        return sums[j, half:window]

    def source(j):
        return sums[j, source_rows]

    def gather_part(side, j, rows):
        owner, p = j // count, j % count
        total = None
        if owner == 1:
            total = parts[p, rows]
        for d in range(owner, m):
            other = lax.rem(mids[side] + d, m)
            remote(
                parts.at[p, rows], parts_in.at[owner, other, p, rows], part_send.at[p, 0],
                part_recv.at[owner, other, p], here,
            ).wait_recv()
            value = parts_in[owner, other, p, rows]
            total = value if total is None else total + value
        return total

    everything = pl.ds(0, nx + columns)
    for side in range(2):
        @pl.when(is_side(side))
        def _():
            for j in range(blocks - 1):
                if early_owner(j) == side:
                    sums[j] = gather_part(side, j, everything)
    for j in range(blocks - 1):
        side = early_owner(j)
        rows = pl.ds((1 - side) * half, window)
        send(
            is_side(side), sums.at[j, rows], sums.at[j, rows],
            sum_send.at[j], sum_recv.at[j], hub(1 - side),
        )

    @pl.when(is_hub)
    def _():
        for side in range(2):
            @pl.when(k == mids[side])
            def _():
                for j in range(blocks - 1):
                    if early_owner(j) != side:
                        rows = pl.ds(side * half, window)
                        remote(
                            sums.at[j, rows], sums.at[j, rows], sum_send.at[j],
                            sum_recv.at[j], here,
                        ).wait_recv()
        prefix[0] = coupling(0)
        prefix_add[0] = source(0)
        for j in range(1, blocks - 1):
            both = exact_dot(
                jnp.concatenate([prefix[j - 1], prefix_add[j - 1]], axis=0), coupling(j)
            )
            prefix[j] = both[:nx]
            prefix_add[j] = both[nx:] + source(j)

        @pl.when(q == 0)
        def _():
            total = None
            for d in range(m):
                remote(
                    opening.at[pl.ds(0, half)], opening_in.at[d], open_send.at[0],
                    open_recv.at[d], here,
                ).wait_recv()
                total = opening_in[d] if total is None else total + opening_in[d]
            states_out[0] = total

        last = blocks - 1
        for side in range(2):
            @pl.when(k == mids[side])
            def _():
                rows = pl.ds(side * half, window)
                sums[last, rows] = gather_part(side, last, rows)
        both = exact_dot(
            jnp.concatenate([prefix[last - 1], prefix_add[last - 1]], axis=0), coupling(last)
        )
        comp[:nx] = both[:nx]
        comp[nx:] = both[nx:] + source(last)

        @pl.when(q == 0)
        def _():
            comp[nx:] = exact_dot(states_out[0], comp[:nx]) + comp[nx:]

    added = pl.ds(nx, half)
    kept = pl.ds(0, nx)
    for d in range(1, chips):
        later = {"chain": 2 * lax.rem(q + d, chips) + 1}
        send(
            is_hub & (q > 0) & (q + d < chips), comp, gathered.at[q], comp_send.at[d - 1],
            comp_recv.at[q], later,
        )
        send(
            is_hub & (q == 0), comp.at[added], gathered.at[q, added], comp_send.at[d - 1],
            comp_recv.at[q], later,
        )

    @pl.when(is_hub)
    def _():
        ahead[...] = tall(
            terms(jnp.concatenate([prefix[j] for j in range(blocks - 1)], axis=1)), 0
        )

        @pl.when(q > 0)
        def _():
            remote(
                comp.at[added], gathered.at[0, added], comp_send.at[0], comp_recv.at[0], here
            ).wait_recv()

            def fold(s, state):
                remote(
                    comp, gathered.at[s], comp_send.at[0], comp_recv.at[s], here
                ).wait_recv()
                return exact_dot(state, gathered[s, :nx]) + gathered[s, nx:]

            states_out[0] = lax.fori_loop(1, q, fold, gathered[0, nx:])

        spread_out = jnp.dot(
            wide(terms(states_out[0])), ahead[...], preferred_element_type=F32
        )
        for j in range(1, blocks):
            states_out[j] = spread_out[:, (j - 1) * nx:j * nx] + prefix_add[j - 1]

    def spread(source_ref, target, sends, recvs, order):
        for p in order:
            for d in range(m):
                to = lax.rem(k + d, m)
                if d > 0:
                    send(
                        is_hub, source_ref.at[count + p], target.at[p, h],
                        sends.at[count + p, d], recvs.at[p, h], {"col": to},
                    )
                send(
                    is_hub, source_ref.at[p], target.at[p, h],
                    sends.at[p, d], recvs.at[p, h], {"chain": 2 * q, "col": to},
                )

            @pl.when(is_hub)
            def _():
                target[p, h] = source_ref[count + p]

    def arrive(target, p, recvs):
        for side in range(2):
            @pl.when(jnp.logical_not(is_side(side)))
            def _():
                remote(
                    target.at[p, side], target.at[p, side], exit_sem.at[0],
                    recvs.at[p, side], here,
                ).wait_recv()

    spread(states_out, states, state_send, state_recv, range(count))

    for d in range(1, chips):
        send(
            is_hub & (q - d >= 0), comp.at[kept], gathered.at[q, kept],
            comp_send.at[chips - 1 + d - 1], comp_recv.at[q],
            {"chain": 2 * lax.rem(q - d + chips, chips) + 1},
        )

    for p in range(count):
        arrive(states, p, state_recv)
        state = states[p].reshape(columns, nx)
        forward[k, p] = (rhs[p].astype(F32) - split_dot_t(state, entry[p])).astype(BF16)
        for way, step in ((0, 1), (1, -1)):
            beyond = k + step
            send(
                (beyond >= 0) & (beyond < m), forward.at[k, p], forward.at[k, p],
                fwd_send.at[k, p, way], fwd_recv.at[k, p], {"col": beyond},
            )

    @pl.when(is_hub)
    def _():
        suffix = [coupling(blocks - 1)]
        for j in range(blocks - 2, 0, -1):
            suffix.append(exact_dot(coupling(j), suffix[-1]))
        after[...] = tall(terms(jnp.concatenate(suffix[::-1], axis=0)), 1)

    def block(j, p):
        return binv[p, :, pl.ds(pl.multiple_of(j * width, 128), width)]

    for p in range(count):
        loads[4 + p].wait()
        applied[p] = dot_t(forward[k, p], block(k, p))
    for d in range(1, m):
        for p in range(count):
            for way, step in ((0, 1), (1, -1)):
                j = k - step * d
                beyond = k + step
                there = (j >= 0) & (j < m)

                @pl.when(there)
                def _():
                    remote(
                        forward.at[j, p], forward.at[j, p], fwd_send.at[j, p, way],
                        fwd_recv.at[j, p], here,
                    ).wait_recv()

                send(
                    there & (beyond >= 0) & (beyond < m),
                    forward.at[j, p], forward.at[j, p],
                    fwd_send.at[j, p, way], fwd_recv.at[j, p], {"col": beyond},
                )
            for step in (1, -1):
                j = k - step * d

                @pl.when((j >= 0) & (j < m))
                def _():
                    applied[p] += dot_t(forward[j, p], block(j, p))
            if d == m - 1:
                carried[p] = jnp.dot(
                    applied[p].astype(BF16), entry[p], preferred_element_type=F32
                )
                for side in range(2):
                    rows = pl.ds(side * half, half)
                    send(
                        jnp.logical_not(is_side(side)), carried.at[p, rows],
                        carried_in.at[core, k, p], car_send.at[p, side],
                        car_recv.at[core, k, p], hub(side),
                    )

    own_rows = pl.ds(pl.multiple_of(h * half, 8), half)

    @pl.when(is_hub)
    def _():
        for j in range(blocks):
            owner, p = j // count, j % count
            total = carried[p, own_rows] if owner == 1 else None
            for d in range(owner, m):
                other = lax.rem(k + d, m)
                remote(
                    carried.at[p, own_rows], carried_in.at[owner, other, p],
                    car_send.at[p, 0], car_recv.at[owner, other, p], here,
                ).wait_recv()
                value = carried_in[owner, other, p]
                total = value if total is None else total + value
            carried_sum[j] = total
        stretched = jnp.concatenate([carried_sum[j] for j in range(1, blocks)], axis=1)
        reach = jnp.concatenate([prefix[j] for j in range(blocks - 1)], axis=1)
        back[...] = exact_dot_t(stretched, reach) + carried_sum[0]

    for d in range(1, chips):
        send(
            is_hub & (q - d >= 0), back, back_in.at[q], back_send.at[d - 1],
            back_recv.at[q], {"chain": 2 * lax.rem(q - d + chips, chips) + 1},
        )

    @pl.when(is_hub)
    def _():
        local[blocks - 2] = carried_sum[blocks - 1]
        for j in range(blocks - 3, -1, -1):
            local[j] = exact_dot_t(local[j + 1], coupling(j + 2 - 1)) + carried_sum[j + 1]

        def fold(i, state):
            s = chips - 1 - i
            remote(
                comp.at[kept], gathered.at[s, kept], comp_send.at[0], comp_recv.at[s], here
            ).wait_recv()
            remote(back, back_in.at[s], back_send.at[0], back_recv.at[s], here).wait_recv()
            return exact_dot_t(state, gathered[s, :nx]) + back_in[s]

        state = lax.fori_loop(0, chips - 1 - q, fold, jnp.zeros((half, nx), F32))
        behind_out[blocks - 1] = state
        spread_out = dot_t(wide(terms(state)), after[...])
        for j in range(blocks - 1):
            behind_out[j] = spread_out[:, j * nx:(j + 1) * nx] + local[j]

    spread(behind_out, behind, beh_send, beh_recv, reversed(range(count)))

    for p in reversed(range(count)):
        arrive(behind, p, beh_recv)
        state = behind[p].reshape(columns, nx)
        out_ref[p] = applied[p] - split_dot_t(state, following(p))

    for condition, args in unsent:
        @pl.when(condition)
        def _():
            remote(*args).wait_send()


def shards(n, m, rhs, block_inverse, entry_factor, exit_factor, previous):
    count, columns, width = rhs.shape
    nx = entry_factor.shape[2]
    padded = -(-width // 128) * 128
    if padded != width:
        extra = padded - width
        rhs = jnp.pad(rhs, ((0, 0), (0, 0), (0, extra)))
        previous = jnp.pad(previous, ((0, 0), (0, extra)))
        entry_factor = jnp.pad(entry_factor, ((0, 0), (0, extra), (0, 0)))
        exit_factor = jnp.pad(exit_factor, ((0, 0), (0, extra), (0, 0)))
        block_inverse = jnp.pad(
            block_inverse.reshape(count, width, m, width),
            ((0, 0), (0, extra), (0, 0), (0, extra)),
        ).reshape(count, padded, m * padded)
    vmem = pltpu.VMEM
    dma = pltpu.SemaphoreType.DMA
    chips = n // 2
    blocks = 2 * count
    half = columns // 2
    rest = blocks - 1
    out = pl.pallas_call(
        functools.partial(kernel, n, m),
        out_shape=jax.ShapeDtypeStruct((count, columns, padded), F32),
        in_specs=[pl.BlockSpec(memory_space=pl.ANY)] * 5,
        out_specs=pl.BlockSpec(memory_space=pltpu.VMEM),
        scratch_shapes=[
            vmem((count, columns, padded), BF16),
            vmem(block_inverse.shape, BF16),
            vmem(entry_factor.shape, BF16),
            vmem(exit_factor.shape, BF16),
            vmem(previous.shape, BF16),
            vmem(exit_factor.shape[1:], BF16),
            vmem((count, nx + columns, nx), F32),
            vmem((2, m, count, nx + columns, nx), F32),
            vmem((columns, nx), F32),
            vmem((m, half, nx), F32),
            vmem((blocks, nx + columns, nx), F32),
            vmem((rest, nx, nx), F32),
            vmem((rest, half, nx), F32),
            vmem((6 * nx, rest * nx), BF16),
            vmem((rest * nx, 6 * nx), BF16),
            vmem((nx + half, nx), F32),
            vmem((chips, nx + half, nx), F32),
            vmem((blocks, half, nx), F32),
            vmem((count, 2, half, nx), F32),
            vmem((m, count, columns, padded), BF16),
            vmem((count, columns, padded), F32),
            vmem((count, columns, nx), F32),
            vmem((2, m, count, half, nx), F32),
            vmem((blocks, half, nx), F32),
            vmem((half, nx), F32),
            vmem((chips, half, nx), F32),
            vmem((rest, half, nx), F32),
            vmem((blocks, half, nx), F32),
            vmem((count, 2, half, nx), F32),
            dma((4 + count,)),
            dma((2,)),
            dma((count, 2)), dma((2, m, count)),
            dma((blocks,)), dma((blocks,)),
            dma((2,)), dma((m,)),
            dma((2 * chips,)), dma((chips,)),
            dma((blocks, m)), dma((count, 2)),
            dma((m, count, 2)), dma((m, count)),
            dma((count, 2)), dma((2, m, count)),
            dma((chips,)), dma((chips,)),
            dma((blocks, m)), dma((count, 2)),
        ],
        compiler_params=pltpu.CompilerParams(
            collective_id=0, has_side_effects=True
        ),
    )(rhs, block_inverse, entry_factor, exit_factor, previous)
    return out[:, :, :width] if padded != width else out


def solution(mesh):
    placed = (
        P("chain", None, "col"),
        P("chain", "col", None),
        P("chain", "col", None),
        P("chain", "col", None),
        P(None, "col"),
    )
    return jax.shard_map(
        functools.partial(shards, mesh.shape["chain"], mesh.shape["col"]),
        mesh=mesh, in_specs=placed, out_specs=P("chain", None, "col"), check_vma=False,
    )
```

```python
import functools

import jax
import jax.numpy as jnp
from jax import lax
from jax.experimental import pallas as pl
from jax.experimental.pallas import tpu as pltpu
from jax.sharding import PartitionSpec as P

MESH = pl.DeviceIdType.MESH
F32 = jnp.float32
BF16 = jnp.bfloat16


def dot_t(a, b):
    return lax.dot_general(a, b, (((1,), (1,)), ((), ())), preferred_element_type=F32)


def terms(x):
    first = x.astype(BF16)
    rest = x - first.astype(F32)
    second = rest.astype(BF16)
    third = (rest - second.astype(F32)).astype(BF16)
    return first, second, third


def split_dot_t(x, low):
    rows = x.shape[0]
    product = dot_t(jnp.concatenate(terms(x), axis=0), low)
    return (product[2 * rows:] + product[rows:2 * rows]) + product[:rows]


def wide(parts):
    a1, a2, a3 = parts
    return jnp.concatenate([a3, a2, a1, a2, a1, a1], axis=1)


def tall(parts, axis):
    b1, b2, b3 = parts
    return jnp.concatenate([b1, b2, b3, b1, b2, b1], axis=axis)


def exact_dot(a, b):
    return jnp.dot(wide(terms(a)), tall(terms(b), 0), preferred_element_type=F32)


def exact_dot_t(a, b):
    return dot_t(wide(terms(a)), tall(terms(b), 1))


def kernel(
    n, m, rhs_hbm, binv_hbm, entry_hbm, exit_hbm, prev_hbm, out_ref,
    rhs, binv, entry, exits, prev, arriving,
    parts, parts_in, opening, opening_in, sums, prefix, prefix_add, ahead, after,
    comp, gathered, states_out, states, forward, applied, carried, carried_in,
    carried_sum, back, back_in, local, behind_out, behind,
    local_sem, exit_sem, part_send, part_recv, open_send, open_recv,
    comp_send, comp_recv, state_send, state_recv, fwd_send, fwd_recv,
    car_send, car_recv, back_send, back_recv, beh_send, beh_recv,
):
    c = lax.axis_index("chain")
    k = lax.axis_index("col")
    count, columns, width = rhs.shape
    nx = entry.shape[2]
    half = columns // 2
    window = nx + half
    chips = n // 2
    q = c // 2
    core = lax.rem(c, 2)
    mids = (m // 2 - 1, m // 2)
    blocks = 2 * count
    h = jnp.clip(k - mids[0], 0, 1)
    is_hub = (core == 1) & (k >= mids[0]) & (k <= mids[1])
    unsent = []

    def hub(side):
        return {"chain": 2 * q + 1, "col": mids[0] + side}

    def is_side(side):
        return (core == 1) & (k == mids[0] + side)

    low = jnp.where(k <= mids[0], 1, 0)
    far_first = (low, 1 - low)

    def remote(src, dst, send, recv, where):
        return pltpu.make_async_remote_copy(
            src_ref=src, dst_ref=dst, send_sem=send, recv_sem=recv,
            device_id=where, device_id_type=MESH,
        )

    def send(condition, *args):
        @pl.when(condition)
        def _():
            remote(*args).start()

        unsent.append((condition, args))

    here = {"chain": c, "col": k}
    loads = [
        pltpu.make_async_copy(exit_hbm, exits, local_sem.at[0]),
        pltpu.make_async_copy(entry_hbm, entry, local_sem.at[1]),
        pltpu.make_async_copy(rhs_hbm, rhs, local_sem.at[2]),
        pltpu.make_async_copy(prev_hbm, prev, local_sem.at[3]),
    ] + [
        pltpu.make_async_copy(binv_hbm.at[p], binv.at[p], local_sem.at[4 + p])
        for p in range(count)
    ]
    for load in loads:
        load.start()

    barrier = pltpu.get_barrier_semaphore()
    for d in range(1, m):
        for other in range(2):
            pl.semaphore_signal(
                barrier, 1, device_id={"chain": 2 * q + other, "col": lax.rem(k + d, m)},
                device_id_type=MESH,
            )
    pl.semaphore_signal(barrier, 1, device_id={"chain": 2 * q + 1 - core}, device_id_type=MESH)

    beside = c + 2 * core - 1
    has_beside = (beside >= 0) & (beside < n)

    @pl.when(has_beside)
    def _():
        pl.semaphore_signal(barrier, 1, device_id={"chain": beside}, device_id_type=MESH)

    @pl.when(is_hub)
    def _():
        for d in range(1, chips):
            pl.semaphore_signal(
                barrier, 1, device_id={"chain": 2 * lax.rem(q + d, chips) + 1},
                device_id_type=MESH,
            )

    @pl.when(c == n - 1)
    def _():
        arriving[...] = jnp.zeros_like(arriving)

    for load in loads[:4]:
        load.wait()

    @pl.when(c == 0)
    def _():
        opening[...] = jnp.dot(prev[...], exits[0], preferred_element_type=F32)

    def following(p):
        return exits[p + 1] if p + 1 < count else arriving[...]

    def part(p):
        after_p = following(p)
        source = jnp.dot(rhs[p], after_p, preferred_element_type=F32)
        parts[p, :half] = source[:half]
        parts[p, half:window] = -lax.dot_general(
            entry[p], after_p, (((0,), (0,)), ((), ())), preferred_element_type=F32
        )
        parts[p, window:] = source[half:]

    for p in range(count - 1):
        part(p)

    expected = 2 * m - 1 + jnp.where(has_beside, 1, 0) + jnp.where(is_hub, chips - 1, 0)
    pl.semaphore_wait(barrier, expected)

    send(c > 0, exits.at[0], arriving, exit_sem.at[0], exit_sem.at[1], {"chain": c - 1})
    for side in range(2):
        send(
            c == 0, opening.at[pl.ds(side * half, half)], opening_in.at[k],
            open_send.at[side], open_recv.at[k], hub(side),
        )

    for p in range(count):
        if p + 1 == count:
            @pl.when(c < n - 1)
            def _():
                remote(
                    exits.at[0], arriving, exit_sem.at[0], exit_sem.at[1], here
                ).wait_recv()
            part(p)
        for side in far_first:
            rows = pl.ds(pl.multiple_of(side * half, 8), window)
            send(
                jnp.logical_not(is_side(side)), parts.at[p, rows],
                parts_in.at[core, k, p, rows], part_send.at[p, side],
                part_recv.at[core, k, p], hub(side),
            )

    mine = pl.ds(pl.multiple_of(h * half, 8), window)
    source_rows = pl.ds(pl.multiple_of(h * window, 8), half)

    def coupling(j):
        return sums[j, half:window]

    def source(j):
        return sums[j, source_rows]

    def gather_part(j):
        owner, p = j // count, j % count
        total = parts[p, mine] if owner == 1 else None
        for d in range(owner, m):
            other = lax.rem(k + d, m)
            remote(
                parts.at[p, mine], parts_in.at[owner, other, p, mine], part_send.at[p, 0],
                part_recv.at[owner, other, p], here,
            ).wait_recv()
            value = parts_in[owner, other, p, mine]
            total = value if total is None else total + value
        sums[j, mine] = total

    @pl.when(is_hub)
    def _():
        gather_part(0)
        prefix[0] = coupling(0)
        prefix_add[0] = source(0)
        for j in range(1, blocks - 1):
            gather_part(j)
            both = exact_dot(
                jnp.concatenate([prefix[j - 1], prefix_add[j - 1]], axis=0), coupling(j)
            )
            prefix[j] = both[:nx]
            prefix_add[j] = both[nx:] + source(j)

        @pl.when(q == 0)
        def _():
            total = None
            for d in range(m):
                remote(
                    opening.at[pl.ds(0, half)], opening_in.at[d], open_send.at[0],
                    open_recv.at[d], here,
                ).wait_recv()
                total = opening_in[d] if total is None else total + opening_in[d]
            states_out[0] = total

        last = blocks - 1
        gather_part(last)
        both = exact_dot(
            jnp.concatenate([prefix[last - 1], prefix_add[last - 1]], axis=0), coupling(last)
        )
        comp[:nx] = both[:nx]
        comp[nx:] = both[nx:] + source(last)

        @pl.when(q == 0)
        def _():
            comp[nx:] = exact_dot(states_out[0], comp[:nx]) + comp[nx:]

    added = pl.ds(nx, half)
    kept = pl.ds(0, nx)
    for d in range(1, chips):
        later = {"chain": 2 * lax.rem(q + d, chips) + 1}
        send(
            is_hub & (q > 0) & (q + d < chips), comp, gathered.at[q], comp_send.at[d - 1],
            comp_recv.at[q], later,
        )
        send(
            is_hub & (q == 0), comp.at[added], gathered.at[q, added], comp_send.at[d - 1],
            comp_recv.at[q], later,
        )

    @pl.when(is_hub)
    def _():
        ahead[...] = tall(
            terms(jnp.concatenate([prefix[j] for j in range(blocks - 1)], axis=1)), 0
        )

        @pl.when(q > 0)
        def _():
            remote(
                comp.at[added], gathered.at[0, added], comp_send.at[0], comp_recv.at[0], here
            ).wait_recv()

            def fold(s, state):
                remote(
                    comp, gathered.at[s], comp_send.at[0], comp_recv.at[s], here
                ).wait_recv()
                return exact_dot(state, gathered[s, :nx]) + gathered[s, nx:]

            states_out[0] = lax.fori_loop(1, q, fold, gathered[0, nx:])

        spread_out = jnp.dot(
            wide(terms(states_out[0])), ahead[...], preferred_element_type=F32
        )
        for j in range(1, blocks):
            states_out[j] = spread_out[:, (j - 1) * nx:j * nx] + prefix_add[j - 1]

    def spread(source_ref, target, sends, recvs, order):
        for p in order:
            for d in range(m):
                to = lax.rem(k + d, m)
                if d > 0:
                    send(
                        is_hub, source_ref.at[count + p], target.at[p, h],
                        sends.at[count + p, d], recvs.at[p, h], {"col": to},
                    )
                send(
                    is_hub, source_ref.at[p], target.at[p, h],
                    sends.at[p, d], recvs.at[p, h], {"chain": 2 * q, "col": to},
                )

            @pl.when(is_hub)
            def _():
                target[p, h] = source_ref[count + p]

    def arrive(target, p, recvs):
        for side in range(2):
            @pl.when(jnp.logical_not(is_side(side)))
            def _():
                remote(
                    target.at[p, side], target.at[p, side], exit_sem.at[0],
                    recvs.at[p, side], here,
                ).wait_recv()

    spread(states_out, states, state_send, state_recv, range(count))

    for d in range(1, chips):
        send(
            is_hub & (q - d >= 0), comp.at[kept], gathered.at[q, kept],
            comp_send.at[chips - 1 + d - 1], comp_recv.at[q],
            {"chain": 2 * lax.rem(q - d + chips, chips) + 1},
        )

    for p in range(count):
        arrive(states, p, state_recv)
        state = states[p].reshape(columns, nx)
        forward[k, p] = (rhs[p].astype(F32) - split_dot_t(state, entry[p])).astype(BF16)
        for way, step in ((0, 1), (1, -1)):
            beyond = k + step
            send(
                (beyond >= 0) & (beyond < m), forward.at[k, p], forward.at[k, p],
                fwd_send.at[k, p, way], fwd_recv.at[k, p], {"col": beyond},
            )

    @pl.when(is_hub)
    def _():
        suffix = [coupling(blocks - 1)]
        for j in range(blocks - 2, 0, -1):
            suffix.append(exact_dot(coupling(j), suffix[-1]))
        after[...] = tall(terms(jnp.concatenate(suffix[::-1], axis=0)), 1)

    def block(j, p):
        return binv[p, :, pl.ds(pl.multiple_of(j * width, 128), width)]

    for p in range(count):
        loads[4 + p].wait()
        applied[p] = dot_t(forward[k, p], block(k, p))
    for d in range(1, m):
        for p in range(count):
            for way, step in ((0, 1), (1, -1)):
                j = k - step * d
                beyond = k + step
                there = (j >= 0) & (j < m)

                @pl.when(there)
                def _():
                    remote(
                        forward.at[j, p], forward.at[j, p], fwd_send.at[j, p, way],
                        fwd_recv.at[j, p], here,
                    ).wait_recv()

                send(
                    there & (beyond >= 0) & (beyond < m),
                    forward.at[j, p], forward.at[j, p],
                    fwd_send.at[j, p, way], fwd_recv.at[j, p], {"col": beyond},
                )
            for step in (1, -1):
                j = k - step * d

                @pl.when((j >= 0) & (j < m))
                def _():
                    applied[p] += dot_t(forward[j, p], block(j, p))
            if d == m - 1:
                carried[p] = jnp.dot(
                    applied[p].astype(BF16), entry[p], preferred_element_type=F32
                )
                for side in far_first:
                    rows = pl.ds(pl.multiple_of(side * half, 8), half)
                    send(
                        jnp.logical_not(is_side(side)), carried.at[p, rows],
                        carried_in.at[core, k, p], car_send.at[p, side],
                        car_recv.at[core, k, p], hub(side),
                    )

    own_rows = pl.ds(pl.multiple_of(h * half, 8), half)

    @pl.when(is_hub)
    def _():
        for j in range(blocks):
            owner, p = j // count, j % count
            total = carried[p, own_rows] if owner == 1 else None
            for d in range(owner, m):
                other = lax.rem(k + d, m)
                remote(
                    carried.at[p, own_rows], carried_in.at[owner, other, p],
                    car_send.at[p, 0], car_recv.at[owner, other, p], here,
                ).wait_recv()
                value = carried_in[owner, other, p]
                total = value if total is None else total + value
            carried_sum[j] = total
        stretched = jnp.concatenate([carried_sum[j] for j in range(1, blocks)], axis=1)
        reach = jnp.concatenate([prefix[j] for j in range(blocks - 1)], axis=1)
        back[...] = exact_dot_t(stretched, reach) + carried_sum[0]

    for d in range(1, chips):
        send(
            is_hub & (q - d >= 0), back, back_in.at[q], back_send.at[d - 1],
            back_recv.at[q], {"chain": 2 * lax.rem(q - d + chips, chips) + 1},
        )

    @pl.when(is_hub)
    def _():
        local[blocks - 2] = carried_sum[blocks - 1]
        for j in range(blocks - 3, -1, -1):
            local[j] = exact_dot_t(local[j + 1], coupling(j + 1)) + carried_sum[j + 1]

        def fold(i, state):
            s = chips - 1 - i
            remote(
                comp.at[kept], gathered.at[s, kept], comp_send.at[0], comp_recv.at[s], here
            ).wait_recv()
            remote(back, back_in.at[s], back_send.at[0], back_recv.at[s], here).wait_recv()
            return exact_dot_t(state, gathered[s, :nx]) + back_in[s]

        state = lax.fori_loop(0, chips - 1 - q, fold, jnp.zeros((half, nx), F32))
        behind_out[blocks - 1] = state
        spread_out = dot_t(wide(terms(state)), after[...])
        for j in range(blocks - 1):
            behind_out[j] = spread_out[:, j * nx:(j + 1) * nx] + local[j]

    spread(behind_out, behind, beh_send, beh_recv, reversed(range(count)))

    for p in reversed(range(count)):
        arrive(behind, p, beh_recv)
        state = behind[p].reshape(columns, nx)
        out_ref[p] = applied[p] - split_dot_t(state, following(p))

    for condition, args in unsent:
        @pl.when(condition)
        def _():
            remote(*args).wait_send()


def shards(n, m, rhs, block_inverse, entry_factor, exit_factor, previous):
    count, columns, width = rhs.shape
    nx = entry_factor.shape[2]
    padded = -(-width // 128) * 128
    if padded != width:
        extra = padded - width
        rhs = jnp.pad(rhs, ((0, 0), (0, 0), (0, extra)))
        previous = jnp.pad(previous, ((0, 0), (0, extra)))
        entry_factor = jnp.pad(entry_factor, ((0, 0), (0, extra), (0, 0)))
        exit_factor = jnp.pad(exit_factor, ((0, 0), (0, extra), (0, 0)))
        block_inverse = jnp.pad(
            block_inverse.reshape(count, width, m, width),
            ((0, 0), (0, extra), (0, 0), (0, extra)),
        ).reshape(count, padded, m * padded)
    vmem = pltpu.VMEM
    dma = pltpu.SemaphoreType.DMA
    chips = n // 2
    blocks = 2 * count
    half = columns // 2
    rest = blocks - 1
    out = pl.pallas_call(
        functools.partial(kernel, n, m),
        out_shape=pltpu.VMEM((count, columns, padded), F32),
        in_specs=[pl.BlockSpec(memory_space=pltpu.HBM)] * 5,
        out_specs=pl.BlockSpec(memory_space=pltpu.VMEM),
        scratch_shapes=[
            vmem((count, columns, padded), BF16),
            vmem(block_inverse.shape, BF16),
            vmem(entry_factor.shape, BF16),
            vmem(exit_factor.shape, BF16),
            vmem(previous.shape, BF16),
            vmem(exit_factor.shape[1:], BF16),
            vmem((count, nx + columns, nx), F32),
            vmem((2, m, count, nx + columns, nx), F32),
            vmem((columns, nx), F32),
            vmem((m, half, nx), F32),
            vmem((blocks, nx + columns, nx), F32),
            vmem((rest, nx, nx), F32),
            vmem((rest, half, nx), F32),
            vmem((6 * nx, rest * nx), BF16),
            vmem((rest * nx, 6 * nx), BF16),
            vmem((nx + half, nx), F32),
            vmem((chips, nx + half, nx), F32),
            vmem((blocks, half, nx), F32),
            vmem((count, 2, half, nx), F32),
            vmem((m, count, columns, padded), BF16),
            vmem((count, columns, padded), F32),
            vmem((count, columns, nx), F32),
            vmem((2, m, count, half, nx), F32),
            vmem((blocks, half, nx), F32),
            vmem((half, nx), F32),
            vmem((chips, half, nx), F32),
            vmem((rest, half, nx), F32),
            vmem((blocks, half, nx), F32),
            vmem((count, 2, half, nx), F32),
            dma((4 + count,)),
            dma((2,)),
            dma((count, 2)), dma((2, m, count)),
            dma((2,)), dma((m,)),
            dma((2 * chips,)), dma((chips,)),
            dma((blocks, m)), dma((count, 2)),
            dma((m, count, 2)), dma((m, count)),
            dma((count, 2)), dma((2, m, count)),
            dma((chips,)), dma((chips,)),
            dma((blocks, m)), dma((count, 2)),
        ],
        compiler_params=pltpu.CompilerParams(
            collective_id=0, has_side_effects=True, vmem_limit_bytes=40 * 2**20
        ),
    )(*(
        pltpu.with_memory_space_constraint(x, pltpu.HBM)
        for x in (rhs, block_inverse, entry_factor, exit_factor, previous)
    ))
    return out[:, :, :width] if padded != width else out


def solution(mesh):
    placed = (
        P("chain", None, "col"),
        P("chain", "col", None),
        P("chain", "col", None),
        P("chain", "col", None),
        P(None, "col"),
    )
    return jax.shard_map(
        functools.partial(shards, mesh.shape["chain"], mesh.shape["col"]),
        mesh=mesh, in_specs=placed, out_specs=P("chain", None, "col"), check_vma=False,
    )
```

```python
import functools

import jax
import jax.numpy as jnp
from jax import lax
from jax.experimental import pallas as pl
from jax.experimental.pallas import tpu as pltpu
from jax.sharding import PartitionSpec as P

MESH = pl.DeviceIdType.MESH
F32 = jnp.float32
BF16 = jnp.bfloat16


def dot_t(a, b):
    return lax.dot_general(a, b, (((1,), (1,)), ((), ())), preferred_element_type=F32)


def terms(x):
    first = x.astype(BF16)
    rest = x - first.astype(F32)
    second = rest.astype(BF16)
    third = (rest - second.astype(F32)).astype(BF16)
    return first, second, third


def split_dot_t(x, low):
    rows = x.shape[0]
    product = dot_t(jnp.concatenate(terms(x), axis=0), low)
    return (product[2 * rows:] + product[rows:2 * rows]) + product[:rows]


def wide(parts):
    a1, a2, a3 = parts
    return jnp.concatenate([a3, a2, a1, a2, a1, a1], axis=1)


def tall(parts, axis):
    b1, b2, b3 = parts
    return jnp.concatenate([b1, b2, b3, b1, b2, b1], axis=axis)


def exact_dot(a, b):
    return jnp.dot(wide(terms(a)), tall(terms(b), 0), preferred_element_type=F32)


def exact_dot_t(a, b):
    return dot_t(wide(terms(a)), tall(terms(b), 1))


def prepared(ref, b):
    for i, term in enumerate(terms(b)):
        ref[i] = term


def stacked(a, b1, b2, b3, product):
    rows = a.shape[0]
    a1, a2, a3 = terms(a)
    y1 = product(jnp.concatenate([a1, a2, a3], axis=0), b1)
    y2 = product(jnp.concatenate([a1, a2], axis=0), b2)
    y3 = product(a1, b3)
    small = (y1[2 * rows:] + y2[rows:]) + y3
    return (small + (y1[rows:2 * rows] + y2[:rows])) + y1[:rows]


def plain(a, b):
    return jnp.dot(a, b, preferred_element_type=F32)


def kernel(
    n, m, rhs_hbm, binv_hbm, entry_hbm, exit_hbm, prev_hbm, out_ref,
    rhs, binv, entry, exits, prev, arriving,
    parts, parts_in, opening, opening_in, sums, prefix, prefix_add, ahead, reach, reach_terms,
    comp, gathered, states_out, states, forward, applied, carried, carried_in,
    carried_sum, back, back_in, behind_out, behind, near_entry, near_rhs,
    local_sem, exit_sem, part_send, part_recv, open_send, open_recv,
    comp_send, comp_recv, state_send, state_recv, fwd_send, fwd_recv,
    car_send, car_recv, back_send, back_recv, beh_send, beh_recv, near_send, near_recv,
):
    c = lax.axis_index("chain")
    k = lax.axis_index("col")
    count, columns, width = rhs.shape
    nx = entry.shape[2]
    half = columns // 2
    window = nx + half
    chips = n // 2
    q = c // 2
    core = lax.rem(c, 2)
    mids = (m // 2 - 1, m // 2)
    blocks = 2 * count
    rest = blocks - 1
    h = jnp.clip(k - mids[0], 0, 1)
    is_hub = (core == 1) & (k >= mids[0]) & (k <= mids[1])
    unsent = []

    def hub(side):
        return {"chain": 2 * q + 1, "col": mids[0] + side}

    def is_side(side):
        return (core == 1) & (k == mids[0] + side)

    low = jnp.where(k <= mids[0], 1, 0)
    far_first = (low, 1 - low)

    def remote(src, dst, send, recv, where):
        return pltpu.make_async_remote_copy(
            src_ref=src, dst_ref=dst, send_sem=send, recv_sem=recv,
            device_id=where, device_id_type=MESH,
        )

    def send(condition, *args):
        @pl.when(condition)
        def _():
            remote(*args).start()

    def sent(condition, ref, semaphore):
        unsent.append((condition, ref, semaphore))

    def received(ref, semaphore):
        remote(ref, ref, exit_sem.at[0], semaphore, here).wait_recv()

    here = {"chain": c, "col": k}
    loads = [
        pltpu.make_async_copy(exit_hbm, exits, local_sem.at[0]),
        pltpu.make_async_copy(entry_hbm, entry, local_sem.at[1]),
        pltpu.make_async_copy(rhs_hbm, rhs, local_sem.at[2]),
        pltpu.make_async_copy(prev_hbm, prev, local_sem.at[3]),
    ] + [
        pltpu.make_async_copy(binv_hbm.at[p], binv.at[p], local_sem.at[4 + p])
        for p in range(count)
    ]
    for load in loads[:4]:
        load.start()

    barrier = pltpu.get_barrier_semaphore()
    for d in range(1, m):
        for other in range(2):
            pl.semaphore_signal(
                barrier, 1, device_id={"chain": 2 * q + other, "col": lax.rem(k + d, m)},
                device_id_type=MESH,
            )
    pl.semaphore_signal(barrier, 1, device_id={"chain": 2 * q + 1 - core}, device_id_type=MESH)

    beside = c + 2 * core - 1
    has_beside = (beside >= 0) & (beside < n)

    @pl.when(has_beside)
    def _():
        pl.semaphore_signal(barrier, 1, device_id={"chain": beside}, device_id_type=MESH)

    @pl.when(is_hub)
    def _():
        for d in range(1, chips):
            pl.semaphore_signal(
                barrier, 1, device_id={"chain": 2 * lax.rem(q + d, chips) + 1},
                device_id_type=MESH,
            )

    @pl.when(c == n - 1)
    def _():
        arriving[...] = jnp.zeros_like(arriving)

    for load in loads[:4]:
        load.wait()
    for load in loads[4:]:
        load.start()

    @pl.when(c == 0)
    def _():
        opening[...] = jnp.dot(prev[...], exits[0], preferred_element_type=F32)

    def following(p):
        return exits[p + 1] if p + 1 < count else arriving[...]

    def part(p):
        after_p = following(p)
        source = jnp.dot(rhs[p], after_p, preferred_element_type=F32)
        parts[p, :half] = source[:half]
        parts[p, half:window] = -lax.dot_general(
            entry[p], after_p, (((0,), (0,)), ((), ())), preferred_element_type=F32
        )
        parts[p, window:] = source[half:]

    for p in range(count - 1):
        part(p)

    expected = 2 * m - 1 + jnp.where(has_beside, 1, 0) + jnp.where(is_hub, chips - 1, 0)
    pl.semaphore_wait(barrier, expected)

    send(c > 0, exits.at[0], arriving, exit_sem.at[0], exit_sem.at[1], {"chain": c - 1})
    sent(c > 0, arriving, exit_sem.at[0])
    for side in range(2):
        send(
            c == 0, opening.at[pl.ds(side * half, half)], opening_in.at[k],
            open_send, open_recv, hub(side),
        )
    sent(c == 0, opening, open_send)

    for p in range(count):
        if p + 1 == count:
            @pl.when(c < n - 1)
            def _():
                received(arriving, exit_sem.at[1])
            part(p)
        for side in far_first:
            rows = pl.ds(pl.multiple_of(side * half, 8), window)
            send(
                jnp.logical_not(is_side(side)), parts.at[p, rows],
                parts_in.at[core, k, p, rows], part_send,
                part_recv.at[core * count + p], hub(side),
            )
    sent(jnp.logical_not(is_hub), parts_in.at[0, pl.ds(0, 2), :, pl.ds(0, window)], part_send)
    sent(is_hub, parts_in.at[0, 0, :, pl.ds(0, window)], part_send)

    is_end = (k == 0) | (k == m - 1)
    for way, (at, to) in enumerate(((m - 2, m - 1), (1, 0))):
        send(k == at, entry, near_entry, near_send.at[way, 0], near_recv.at[0], {"col": to})
        send(k == at, rhs, near_rhs, near_send.at[way, 1], near_recv.at[1], {"col": to})
        sent(k == at, entry, near_send.at[way, 0])
        sent(k == at, rhs, near_send.at[way, 1])

    mine = pl.ds(pl.multiple_of(h * half, 8), window)
    source_rows = pl.ds(pl.multiple_of(h * window, 8), half)

    def coupling(j):
        return sums[j, half:window]

    def source(j):
        return sums[j, source_rows]

    def gather_part(j):
        owner, p = j // count, j % count
        received(parts_in.at[owner, pl.ds(0, m - owner), p, mine], part_recv.at[j])
        total = parts[p, mine] if owner == 1 else None
        for d in range(owner, m):
            value = parts_in[owner, lax.rem(k + d, m), p, mine]
            total = value if total is None else total + value
        sums[j, mine] = total

    @pl.when(is_hub)
    def _():
        gather_part(0)
        prefix[0] = coupling(0)
        prefix_add[0] = source(0)
        for j in range(1, blocks - 1):
            gather_part(j)
            both = exact_dot(
                jnp.concatenate([prefix[j - 1], prefix_add[j - 1]], axis=0), coupling(j)
            )
            prefix[j] = both[:nx]
            prefix_add[j] = both[nx:] + source(j)

        @pl.when(q == 0)
        def _():
            received(opening_in, open_recv)
            total = opening_in[0]
            for d in range(1, m):
                total += opening_in[d]
            states_out[0] = total

        last = blocks - 1
        gather_part(last)
        both = exact_dot(
            jnp.concatenate([prefix[last - 1], prefix_add[last - 1]], axis=0), coupling(last)
        )
        comp[:nx] = both[:nx]
        comp[nx:] = both[nx:] + source(last)

        @pl.when(q == 0)
        def _():
            comp[nx:] = exact_dot(states_out[0], comp[:nx]) + comp[nx:]

    added = pl.ds(nx, half)
    kept = pl.ds(0, nx)
    for d in range(1, chips):
        to = lax.rem(q + d, chips)
        later = {"chain": 2 * to + 1}
        send(
            is_hub & (q > 0) & (q + d < chips), comp, gathered.at[q], comp_send.at[to],
            comp_recv.at[q], later,
        )
        sent(is_hub & (q > 0) & (q + d < chips), comp, comp_send.at[to])
        send(
            is_hub & (q == 0), comp.at[added], gathered.at[q, added], comp_send.at[to],
            comp_recv.at[q], later,
        )
        sent(is_hub & (q == 0), comp.at[added], comp_send.at[to])

    @pl.when(is_hub)
    def _():
        prepared(ahead, jnp.concatenate([prefix[j] for j in range(blocks - 1)], axis=1))

        @pl.when(q > 0)
        def _():
            received(gathered.at[0, added], comp_recv.at[0])

            def fold(s, state):
                received(gathered.at[s], comp_recv.at[s])
                return exact_dot(state, gathered[s, :nx]) + gathered[s, nx:]

            states_out[0] = lax.fori_loop(1, q, fold, gathered[0, nx:])

        spread_out = stacked(states_out[0], ahead[0], ahead[1], ahead[2], plain)
        for j in range(1, blocks):
            states_out[j] = spread_out[:, (j - 1) * nx:j * nx] + prefix_add[j - 1]

    def spread(source_ref, target, sends, recvs, order):
        for p in order:
            for i in range(m):
                to = jnp.where(h == 0, m - 1 - i, i)
                send(
                    is_hub, source_ref.at[p], target.at[p, h],
                    sends.at[0], recvs.at[p], {"chain": 2 * q, "col": to},
                )
                send(
                    is_hub & (to != k), source_ref.at[count + p], target.at[p, h],
                    sends.at[1], recvs.at[p], {"col": to},
                )

            @pl.when(is_hub)
            def _():
                target[p, h] = source_ref[count + p]

        sent(is_hub, carried_in.at[0, pl.ds(0, m - 1)], sends.at[1])
        sent(is_hub, carried_in.at[0], sends.at[0])

    def arrive(target, p, recvs):
        @pl.when(is_hub)
        def _():
            received(target.at[p, 0], recvs.at[p])

        @pl.when(jnp.logical_not(is_hub))
        def _():
            received(target.at[p], recvs.at[p])

    spread(states_out, states, state_send, state_recv, range(count))

    for d in range(1, chips):
        to = lax.rem(q - d + chips, chips)
        send(
            is_hub & (q - d >= 0), comp.at[kept], gathered.at[q, kept],
            comp_send.at[to], comp_recv.at[q], {"chain": 2 * to + 1},
        )
        sent(is_hub & (q - d >= 0), comp.at[kept], comp_send.at[to])

    halves = [pl.ds(side * half, half) for side in range(2)]

    def leave(p, condition):
        for way, step in ((0, 1), (1, -1)):
            beyond = k + step
            goes = (beyond >= 0) & (beyond < m) & jnp.logical_not(is_last(beyond))
            for side, rows in enumerate(halves):
                send(
                    goes & condition, forward.at[k, p, rows], forward.at[k, p, rows],
                    fwd_send.at[way], fwd_recv.at[k, p, side], {"col": beyond},
                )

    def is_last(position):
        return (position == 0) | (position == m - 1)

    for place in range(m):
        for way in range(2):
            last = (m - 1, 0)[way]
            if place == last:
                continue
            passed = (place + 1, m - place)[way]
            beside_last = abs(place - last) == 1
            if m > 3 and False:
                for side in range(2):
                    amount = passed - beside_last
                    if side == 0:
                        amount += (passed == 1) - (passed == m - 1)
                    if amount > 0:
                        sent(
                            (k == place) & (core == side), forward.at[pl.ds(0, amount)],
                            fwd_send.at[way],
                        )
            elif passed > beside_last:
                sent(k == place, forward.at[pl.ds(0, passed - beside_last)], fwd_send.at[way])

    for p in range(count):
        arrive(states, p, state_recv)
        state = states[p].reshape(columns, nx)
        forward[k, p] = (rhs[p].astype(F32) - split_dot_t(state, entry[p])).astype(BF16)
        leave(p, core == 0)

    def block(j, p):
        return binv[p, :, pl.ds(pl.multiple_of(j * width, 128), width)]

    for p in range(count):
        loads[4 + p].wait()
        applied[p] = dot_t(forward[k, p], block(k, p))
        leave(p, core == 1)
    near = jnp.where(k == 0, 1, m - 2)

    @pl.when(is_end)
    def _():
        received(near_entry, near_recv.at[0])
        received(near_rhs, near_recv.at[1])
        for p in range(count):
            state = states[p].reshape(columns, nx)
            near_block = near_rhs[p].astype(F32) - split_dot_t(state, near_entry[p])
            applied[p] += dot_t(near_block.astype(BF16), block(near, p))

    def come(d, p):
        for side, rows in enumerate(halves):
            for way, step in ((0, 1), (1, -1)):
                j = k - step * d
                beyond = k + step
                there = (j >= 0) & (j < m)
                if d == 1:
                    there &= jnp.logical_not(is_last(k))

                @pl.when(there)
                def _():
                    received(forward.at[j, p, rows], fwd_recv.at[j, p, side])

                if d + 1 < m:
                    send(
                        there & (beyond >= 0) & (beyond < m),
                        forward.at[j, p, rows], forward.at[j, p, rows],
                        fwd_send.at[way], fwd_recv.at[j, p, side], {"col": beyond},
                    )

    for d in range(1, m - 1):
        for p in range(count):
            come(d, p)
    for d in range(1, m):
        for p in range(count):
            if d + 1 == m:
                come(d, p)
            for step in (1, -1):
                j = k - step * d
                there = (j >= 0) & (j < m)
                if d == 1:
                    there &= jnp.logical_not(is_last(k))

                @pl.when(there)
                def _():
                    applied[p] += dot_t(forward[j, p], block(j, p))
            if d == m - 1:
                carried[p] = jnp.dot(
                    applied[p].astype(BF16), entry[p], preferred_element_type=F32
                )
                for side in far_first:
                    rows = pl.ds(pl.multiple_of(side * half, 8), half)
                    send(
                        jnp.logical_not(is_side(side)), carried.at[p, rows],
                        carried_in.at[core, k, p], car_send,
                        car_recv.at[core * count + p], hub(side),
                    )
    sent(jnp.logical_not(is_hub), carried_in.at[0, pl.ds(0, 2)], car_send)
    sent(is_hub, carried_in.at[0, 0], car_send)

    own_rows = pl.ds(pl.multiple_of(h * half, 8), half)

    @pl.when(is_hub)
    def _():
        suffix = [coupling(blocks - 1)]
        for j in range(blocks - 2, 0, -1):
            suffix.append(exact_dot(coupling(j), suffix[-1]))
        same = lax.broadcasted_iota(jnp.int32, (nx, nx), 0) == lax.broadcasted_iota(
            jnp.int32, (nx, nx), 1
        )
        reach[...] = jnp.concatenate(suffix[::-1] + [jnp.where(same, 1.0, 0.0)], axis=0)

        def extend(s, carry):
            at = pl.ds(pl.multiple_of((s - 1) * nx, 128), nx)
            for i, term in enumerate(terms(reach[...])):
                reach_terms[i, :, at] = term
            received(gathered.at[s, kept], comp_recv.at[s])
            reach[...] = exact_dot(reach[...], gathered[s, :nx])
            return carry

        reach_terms[...] = jnp.zeros_like(reach_terms)
        lax.fori_loop(q + 1, chips, extend, 0)

    @pl.when(is_hub)
    def _():
        offset = None
        for p in range(count):
            for owner in (1, 0):
                j = owner * count + p
                received(carried_in.at[owner, pl.ds(0, m - owner), p], car_recv.at[j])
                total = carried[p, own_rows] if owner == 1 else None
                for d in range(owner, m):
                    value = carried_in[owner, lax.rem(k + d, m), p]
                    total = value if total is None else total + value
                carried_sum[j] = total
                if j > 0:
                    at = slice((j - 1) * nx, j * nx)
                    total = stacked(
                        total, ahead[0, :, at], ahead[1, :, at], ahead[2, :, at], dot_t
                    )
                offset = total if offset is None else offset + total
        back[...] = offset

    for d in range(1, chips):
        to = lax.rem(q - d + chips, chips)
        send(
            is_hub & (q - d >= 0), back, back_in.at[q], back_send.at[d - 1],
            back_recv.at[q], {"chain": 2 * to + 1},
        )
        sent(is_hub & (q - d >= 0), back, back_send.at[d - 1])

    @pl.when(is_hub)
    def _():
        behind_out[blocks - 1] = jnp.zeros((half, nx), F32)
        behind_out[blocks - 2] = carried_sum[blocks - 1]
        for j in range(blocks - 3, -1, -1):
            behind_out[j] = exact_dot_t(behind_out[j + 1], coupling(j + 1)) + carried_sum[j + 1]

        for s in range(1, chips):
            @pl.when(s > q)
            def _():
                received(back_in.at[s], back_recv.at[s])

            @pl.when(s <= q)
            def _():
                back_in[s] = jnp.zeros((half, nx), F32)

        more = stacked(
            jnp.concatenate([back_in[s] for s in range(1, chips)], axis=1),
            reach_terms[0], reach_terms[1], reach_terms[2], dot_t,
        )
        for j in range(blocks):
            behind_out[j] += more[:, j * nx:(j + 1) * nx]

    spread(behind_out, behind, beh_send, beh_recv, reversed(range(count)))

    for p in reversed(range(count)):
        arrive(behind, p, beh_recv)
        state = behind[p].reshape(columns, nx)
        out_ref[p] = applied[p] - split_dot_t(state, following(p))

    for condition, ref, semaphore in unsent:
        @pl.when(condition)
        def _():
            remote(ref, ref, semaphore, semaphore, here).wait_send()


def shards(n, m, rhs, block_inverse, entry_factor, exit_factor, previous):
    count, columns, width = rhs.shape
    nx = entry_factor.shape[2]
    padded = -(-width // 128) * 128
    if padded != width:
        extra = padded - width
        rhs = jnp.pad(rhs, ((0, 0), (0, 0), (0, extra)))
        previous = jnp.pad(previous, ((0, 0), (0, extra)))
        entry_factor = jnp.pad(entry_factor, ((0, 0), (0, extra), (0, 0)))
        exit_factor = jnp.pad(exit_factor, ((0, 0), (0, extra), (0, 0)))
        block_inverse = jnp.pad(
            block_inverse.reshape(count, width, m, width),
            ((0, 0), (0, extra), (0, 0), (0, extra)),
        ).reshape(count, padded, m * padded)
    vmem = pltpu.VMEM
    dma = pltpu.SemaphoreType.DMA
    chips = n // 2
    blocks = 2 * count
    half = columns // 2
    rest = blocks - 1
    out = pl.pallas_call(
        functools.partial(kernel, n, m),
        out_shape=pltpu.VMEM((count, columns, padded), F32),
        in_specs=[pl.BlockSpec(memory_space=pltpu.HBM)] * 5,
        out_specs=pl.BlockSpec(memory_space=pltpu.VMEM),
        scratch_shapes=[
            vmem((count, columns, padded), BF16),
            vmem(block_inverse.shape, BF16),
            vmem(entry_factor.shape, BF16),
            vmem(exit_factor.shape, BF16),
            vmem(previous.shape, BF16),
            vmem(exit_factor.shape[1:], BF16),
            vmem((count, nx + columns, nx), F32),
            vmem((2, m, count, nx + columns, nx), F32),
            vmem((columns, nx), F32),
            vmem((m, half, nx), F32),
            vmem((blocks, nx + columns, nx), F32),
            vmem((rest, nx, nx), F32),
            vmem((rest, half, nx), F32),
            vmem((3, nx, rest * nx), BF16),
            vmem((blocks * nx, nx), F32),
            vmem((3, blocks * nx, (chips - 1) * nx), BF16),
            vmem((nx + half, nx), F32),
            vmem((chips, nx + half, nx), F32),
            vmem((blocks, half, nx), F32),
            vmem((count, 2, half, nx), F32),
            vmem((m, count, columns, padded), BF16),
            vmem((count, columns, padded), F32),
            vmem((count, columns, nx), F32),
            vmem((2, m, count, half, nx), F32),
            vmem((blocks, half, nx), F32),
            vmem((half, nx), F32),
            vmem((chips, half, nx), F32),
            vmem((blocks, half, nx), F32),
            vmem((count, 2, half, nx), F32),
            vmem(entry_factor.shape, BF16),
            vmem((count, columns, padded), BF16),
            dma((4 + count,)),
            dma((2,)),
            dma(()), dma((blocks,)),
            dma(()), dma(()),
            dma((chips,)), dma((chips,)),
            dma((2,)), dma((count,)),
            dma((2,)), dma((m, count, 2)),
            dma(()), dma((blocks,)),
            dma((chips - 1,)), dma((chips,)),
            dma((2,)), dma((count,)),
            dma((2, 2)), dma((2,)),
        ],
        compiler_params=pltpu.CompilerParams(
            collective_id=0, has_side_effects=True, vmem_limit_bytes=40 * 2**20
        ),
    )(*(
        pltpu.with_memory_space_constraint(x, pltpu.HBM)
        for x in (rhs, block_inverse, entry_factor, exit_factor, previous)
    ))
    return out[:, :, :width] if padded != width else out


def solution(mesh):
    placed = (
        P("chain", None, "col"),
        P("chain", "col", None),
        P("chain", "col", None),
        P("chain", "col", None),
        P(None, "col"),
    )
    return jax.shard_map(
        functools.partial(shards, mesh.shape["chain"], mesh.shape["col"]),
        mesh=mesh, in_specs=placed, out_specs=P("chain", None, "col"), check_vma=False,
    )
```

```python
import functools

import jax
import jax.numpy as jnp
from jax import lax
from jax.experimental import pallas as pl
from jax.experimental.pallas import tpu as pltpu
from jax.sharding import PartitionSpec as P

MESH = pl.DeviceIdType.MESH
F32 = jnp.float32
BF16 = jnp.bfloat16


def dot_t(a, b):
    return lax.dot_general(a, b, (((1,), (1,)), ((), ())), preferred_element_type=F32)


def terms(x):
    first = x.astype(BF16)
    rest = x - first.astype(F32)
    second = rest.astype(BF16)
    third = (rest - second.astype(F32)).astype(BF16)
    return first, second, third


def split_dot_t(x, low):
    rows = x.shape[0]
    product = dot_t(jnp.concatenate(terms(x), axis=0), low)
    return (product[2 * rows:] + product[rows:2 * rows]) + product[:rows]


def wide(parts):
    a1, a2, a3 = parts
    return jnp.concatenate([a3, a2, a1, a2, a1, a1], axis=1)


def tall(parts, axis):
    b1, b2, b3 = parts
    return jnp.concatenate([b1, b2, b3, b1, b2, b1], axis=axis)


def exact_dot(a, b):
    return jnp.dot(wide(terms(a)), tall(terms(b), 0), preferred_element_type=F32)


def exact_dot_t(a, b):
    return dot_t(wide(terms(a)), tall(terms(b), 1))


def prepared(ref, b):
    for i, term in enumerate(terms(b)):
        ref[i] = term


def stacked(a, b1, b2, b3, product):
    rows = a.shape[0]
    a1, a2, a3 = terms(a)
    y1 = product(jnp.concatenate([a1, a2, a3], axis=0), b1)
    y2 = product(jnp.concatenate([a1, a2], axis=0), b2)
    y3 = product(a1, b3)
    small = (y1[2 * rows:] + y2[rows:]) + y3
    return (small + (y1[rows:2 * rows] + y2[:rows])) + y1[:rows]


def plain(a, b):
    return jnp.dot(a, b, preferred_element_type=F32)


def kernel(
    n, m, rhs_hbm, binv_hbm, entry_hbm, exit_hbm, prev_hbm, out_ref,
    rhs, binv, entry, exits, prev, arriving,
    parts, parts_in, opening, opening_in, sums, prefix, prefix_add, ahead, reach, reach_terms,
    comp, gathered, states_out, states, forward, applied, carried, carried_in,
    carried_sum, offset, back_in, back_sum, behind_out, behind, own_coupling, own_carried,
    local_sem, exit_sem, part_send, part_recv, open_send, open_recv,
    comp_send, comp_recv, state_send, state_recv, fwd_send, fwd_recv,
    car_send, car_recv, back_send, back_recv, beh_send, beh_recv,
    coup_send, coup_recv, sum_send, sum_recv,
):
    c = lax.axis_index("chain")
    k = lax.axis_index("col")
    count, columns, width = rhs.shape
    nx = entry.shape[2]
    half = columns // 2
    window = nx + half
    chips = n // 2
    q = c // 2
    core = lax.rem(c, 2)
    mids = (m // 2 - 1, m // 2)
    blocks = 2 * count
    rest = blocks - 1
    h = jnp.clip(k - mids[0], 0, 1)
    is_hub = (core == 1) & (k >= mids[0]) & (k <= mids[1])
    unsent = []

    def hub(side):
        return {"chain": 2 * q + 1, "col": mids[0] + side}

    def is_side(side):
        return (core == 1) & (k == mids[0] + side)

    low = jnp.where(k <= mids[0], 1, 0)
    far_first = (low, 1 - low)

    def remote(src, dst, send, recv, where):
        return pltpu.make_async_remote_copy(
            src_ref=src, dst_ref=dst, send_sem=send, recv_sem=recv,
            device_id=where, device_id_type=MESH,
        )

    def send(condition, *args):
        @pl.when(condition)
        def _():
            remote(*args).start()

    def sent(condition, ref, semaphore):
        unsent.append((condition, ref, semaphore))

    def received(ref, semaphore):
        remote(ref, ref, exit_sem.at[0], semaphore, here).wait_recv()

    here = {"chain": c, "col": k}
    loads = [
        pltpu.make_async_copy(exit_hbm, exits, local_sem.at[0]),
        pltpu.make_async_copy(entry_hbm, entry, local_sem.at[1]),
        pltpu.make_async_copy(rhs_hbm, rhs, local_sem.at[2]),
        pltpu.make_async_copy(prev_hbm, prev, local_sem.at[3]),
    ] + [
        pltpu.make_async_copy(binv_hbm.at[p], binv.at[p], local_sem.at[4 + p])
        for p in range(count)
    ]
    for load in loads[:4]:
        load.start()

    barrier = pltpu.get_barrier_semaphore()
    for d in range(1, m):
        for other in range(2):
            pl.semaphore_signal(
                barrier, 1, device_id={"chain": 2 * q + other, "col": lax.rem(k + d, m)},
                device_id_type=MESH,
            )
    pl.semaphore_signal(barrier, 1, device_id={"chain": 2 * q + 1 - core}, device_id_type=MESH)

    beside = c + 2 * core - 1
    has_beside = (beside >= 0) & (beside < n)

    @pl.when(has_beside)
    def _():
        pl.semaphore_signal(barrier, 1, device_id={"chain": beside}, device_id_type=MESH)

    @pl.when(is_hub)
    def _():
        for d in range(1, chips):
            pl.semaphore_signal(
                barrier, 1, device_id={"chain": 2 * lax.rem(q + d, chips) + 1},
                device_id_type=MESH,
            )

    for d in range(1, chips):
        @pl.when(is_hub & (q + d < chips))
        def _():
            for other in range(2):
                for place in range(m):
                    pl.semaphore_signal(
                        barrier, 1, device_id={"chain": 2 * (q + d) + other, "col": place},
                        device_id_type=MESH,
                    )

    @pl.when(c == n - 1)
    def _():
        arriving[...] = jnp.zeros_like(arriving)

    for load in loads[:4]:
        load.wait()
    for load in loads[4:]:
        load.start()

    @pl.when(c == 0)
    def _():
        opening[...] = jnp.dot(prev[...], exits[0], preferred_element_type=F32)

    def following(p):
        return exits[p + 1] if p + 1 < count else arriving[...]

    def part(p):
        after_p = following(p)
        source = jnp.dot(rhs[p], after_p, preferred_element_type=F32)
        parts[p, :half] = source[:half]
        parts[p, half:window] = -lax.dot_general(
            entry[p], after_p, (((0,), (0,)), ((), ())), preferred_element_type=F32
        )
        parts[p, window:] = source[half:]

    for p in range(count - 1):
        part(p)

    expected = 2 * q + 2 * m - 1 + jnp.where(has_beside, 1, 0) + jnp.where(is_hub, chips - 1, 0)
    pl.semaphore_wait(barrier, expected)

    send(c > 0, exits.at[0], arriving, exit_sem.at[0], exit_sem.at[1], {"chain": c - 1})
    sent(c > 0, arriving, exit_sem.at[0])
    for side in range(2):
        send(
            c == 0, opening.at[pl.ds(side * half, half)], opening_in.at[k],
            open_send, open_recv, hub(side),
        )
    sent(c == 0, opening, open_send)

    for p in range(count):
        if p + 1 == count:
            @pl.when(c < n - 1)
            def _():
                received(arriving, exit_sem.at[1])
            part(p)
        for side in far_first:
            rows = pl.ds(pl.multiple_of(side * half, 8), window)
            send(
                jnp.logical_not(is_side(side)), parts.at[p, rows],
                parts_in.at[core, k, p, rows], part_send,
                part_recv.at[core * count + p], hub(side),
            )
    sent(jnp.logical_not(is_hub), parts_in.at[0, pl.ds(0, 2), :, pl.ds(0, window)], part_send)
    sent(is_hub, parts_in.at[0, 0, :, pl.ds(0, window)], part_send)

    added = pl.ds(0, half)
    through = pl.ds(half, nx)
    first_core = pl.ds(window, nx)
    onward = pl.ds(0, window)
    kept = pl.ds(half, 2 * nx)
    mine = pl.ds(pl.multiple_of(h * half, 8), window)
    source_rows = pl.ds(pl.multiple_of(h * window, 8), half)

    def coupling(j):
        return sums[j, half:window]

    def source(j):
        return sums[j, source_rows]

    def gather_part(j):
        owner, p = j // count, j % count
        received(parts_in.at[owner, pl.ds(0, m - owner), p, mine], part_recv.at[j])
        total = parts[p, mine] if owner == 1 else None
        for d in range(owner, m):
            value = parts_in[owner, lax.rem(k + d, m), p, mine]
            total = value if total is None else total + value
        sums[j, mine] = total

    @pl.when(is_hub)
    def _():
        gather_part(0)
        prefix[0] = coupling(0)
        prefix_add[0] = source(0)
        for j in range(1, blocks - 1):
            gather_part(j)
            both = exact_dot(
                jnp.concatenate([prefix[j - 1], prefix_add[j - 1]], axis=0), coupling(j)
            )
            prefix[j] = both[:nx]
            prefix_add[j] = both[nx:] + source(j)

        @pl.when(q == 0)
        def _():
            received(opening_in, open_recv)
            total = opening_in[0]
            for d in range(1, m):
                total += opening_in[d]
            states_out[0] = total

        last = blocks - 1
        gather_part(last)
        both = exact_dot(
            jnp.concatenate([prefix[last - 1], prefix_add[last - 1]], axis=0), coupling(last)
        )
        comp[through] = both[:nx]
        comp[added] = both[nx:] + source(last)
        comp[first_core] = prefix[count - 1]

        @pl.when(q == 0)
        def _():
            comp[added] = exact_dot(states_out[0], comp[through]) + comp[added]

    for d in range(1, chips):
        to = lax.rem(q + d, chips)
        later = {"chain": 2 * to + 1}
        send(
            is_hub & (q > 0) & (q + d < chips), comp.at[onward], gathered.at[q, onward],
            comp_send.at[to], comp_recv.at[q], later,
        )
        sent(is_hub & (q > 0) & (q + d < chips), comp.at[onward], comp_send.at[to])
        send(
            is_hub & (q == 0), comp.at[added], gathered.at[q, added], comp_send.at[to],
            comp_recv.at[q], later,
        )
        sent(is_hub & (q == 0), comp.at[added], comp_send.at[to])

    def spread(condition, source_at, target_at, sends, recv_at, order):
        for p in order:
            for i in range(m):
                to = jnp.where(h == 0, m - 1 - i, i)
                send(
                    condition, source_at(0, p), target_at(p), sends.at[0], recv_at(p),
                    {"chain": 2 * q, "col": to},
                )
                send(
                    condition & (to != k), source_at(1, p), target_at(p), sends.at[1],
                    recv_at(p), {"col": to},
                )

            @pl.when(condition)
            def _():
                target_at(p)[...] = source_at(1, p)[...]

    def spread_sent(condition, sends, amount):
        for owner, places in ((0, m), (1, m - 1)):
            sent(
                condition, carried_in.at[0, pl.ds(0, places), pl.ds(0, amount)],
                sends.at[owner],
            )

    inner = range(1, count)
    quarter = nx // 2
    at_end = q == 0
    shift = jnp.where(at_end, 1, 0)
    spread(
        is_hub,
        lambda owner, i: sums.at[
            owner * count + i + shift, pl.ds(pl.multiple_of(half + h * quarter, 8), quarter)
        ],
        lambda i: own_coupling.at[i, pl.ds(pl.multiple_of(h * quarter, 8), quarter)],
        coup_send, lambda i: coup_recv.at[i], range(count - 1),
    )
    if count > 1:
        for owner, places in ((0, m), (1, m - 1)):
            sent(
                is_hub,
                parts_in.at[0, pl.ds(0, places), pl.ds(0, count - 1), pl.ds(0, quarter)],
                coup_send.at[owner],
            )

    def couplings_arrive():
        for i in range(count - 1):
            @pl.when(is_hub)
            def _():
                received(own_coupling.at[i, pl.ds(0, quarter)], coup_recv.at[i])

            @pl.when(jnp.logical_not(is_hub))
            def _():
                received(own_coupling.at[i], coup_recv.at[i])

    @pl.when(is_hub)
    def _():
        prepared(ahead, jnp.concatenate([prefix[j] for j in range(blocks - 1)], axis=1))

        @pl.when(q > 0)
        def _():
            received(gathered.at[0, added], comp_recv.at[0])

            def fold(s, state):
                received(gathered.at[s, onward], comp_recv.at[s])
                return exact_dot(state, gathered[s, through]) + gathered[s, added]

            states_out[0] = lax.fori_loop(1, q, fold, gathered[0, added])

        spread_out = stacked(states_out[0], ahead[0], ahead[1], ahead[2], plain)
        for j in range(1, blocks):
            states_out[j] = spread_out[:, (j - 1) * nx:j * nx] + prefix_add[j - 1]

    def arrive(target, p, semaphore):
        @pl.when(is_hub)
        def _():
            received(target.at[p, 0], semaphore)

        @pl.when(jnp.logical_not(is_hub))
        def _():
            received(target.at[p], semaphore)

    spread(
        is_hub, lambda owner, p: states_out.at[owner * count + p],
        lambda p: states.at[p, h], state_send, lambda p: state_recv.at[p], range(count),
    )
    spread_sent(is_hub, state_send, count)

    for d in range(1, chips):
        to = lax.rem(q - d + chips, chips)
        send(
            is_hub & (q - d >= 0), comp.at[kept], gathered.at[q, kept],
            comp_send.at[to], comp_recv.at[q], {"chain": 2 * to + 1},
        )
        sent(is_hub & (q - d >= 0), comp.at[kept], comp_send.at[to])

    halves = [pl.ds(side * half, half) for side in range(2)]

    def leave(p, condition):
        for way, step in ((0, 1), (1, -1)):
            beyond = k + step
            goes = (beyond >= 0) & (beyond < m)
            for side, rows in enumerate(halves):
                send(
                    goes & condition, forward.at[k, p, rows], forward.at[k, p, rows],
                    fwd_send.at[way], fwd_recv.at[k, p, side], {"col": beyond},
                )

    for place in range(m):
        if place < m - 1:
            sent(k == place, forward.at[pl.ds(0, place + 1)], fwd_send.at[0])
        if place > 0:
            sent(k == place, forward.at[pl.ds(0, m - place)], fwd_send.at[1])

    for p in range(count):
        arrive(states, p, state_recv.at[p])
        state = states[p].reshape(columns, nx)
        forward[k, p] = (rhs[p].astype(F32) - split_dot_t(state, entry[p])).astype(BF16)
        leave(p, core == 0)

    def block(j, p):
        return binv[p, :, pl.ds(pl.multiple_of(j * width, 128), width)]

    for p in range(count):
        loads[4 + p].wait()
        applied[p] = dot_t(forward[k, p], block(k, p))
        leave(p, core == 1)
    def come(d, p):
        for side, rows in enumerate(halves):
            for way, step in ((0, 1), (1, -1)):
                j = k - step * d
                beyond = k + step
                there = (j >= 0) & (j < m)

                @pl.when(there)
                def _():
                    received(forward.at[j, p, rows], fwd_recv.at[j, p, side])

                if d + 1 < m:
                    send(
                        there & (beyond >= 0) & (beyond < m),
                        forward.at[j, p, rows], forward.at[j, p, rows],
                        fwd_send.at[way], fwd_recv.at[j, p, side], {"col": beyond},
                    )

    for d in range(1, m - 1):
        for p in range(count):
            come(d, p)
    for d in range(1, m):
        for p in range(count):
            if d + 1 == m:
                come(d, p)
            for step in (1, -1):
                j = k - step * d
                there = (j >= 0) & (j < m)

                @pl.when(there)
                def _():
                    applied[p] += dot_t(forward[j, p], block(j, p))
            if d == m - 1:
                carried[p] = jnp.dot(
                    applied[p].astype(BF16), entry[p], preferred_element_type=F32
                )
                for side in far_first:
                    rows = pl.ds(pl.multiple_of(side * half, 8), half)
                    send(
                        jnp.logical_not(is_side(side)), carried.at[p, rows],
                        carried_in.at[core, k, p], car_send,
                        car_recv.at[core * count + p], hub(side),
                    )
    sent(jnp.logical_not(is_hub), carried_in.at[0, pl.ds(0, 2)], car_send)
    sent(is_hub, carried_in.at[0, 0], car_send)

    @pl.when(jnp.logical_not(at_end))
    def _():
        couplings_arrive()
        term = carried[count - 1]
        for p in range(count - 2, -1, -1):
            term = exact_dot_t(term, own_coupling[p]) + carried[p]
        offset[...] = term

    for t in range(chips - 1):
        for side in far_first:
            send(
                t < q, offset.at[pl.ds(pl.multiple_of(side * half, 8), half)],
                back_in.at[c, k], back_send, back_recv.at[c],
                {"chain": 2 * t + 1, "col": mids[0] + side},
            )
        sent(q == t + 1, back_in.at[pl.ds(0, t + 1), pl.ds(0, 2)], back_send)

    own_rows = pl.ds(pl.multiple_of(h * half, 8), half)

    others = [j for j in range(blocks - 1) if j != count - 1]

    @pl.when(is_hub)
    def _():
        suffix = [coupling(blocks - 1)]
        for j in range(blocks - 2, 0, -1):
            suffix.append(exact_dot(coupling(j), suffix[-1]))
        suffix = suffix[::-1]
        same = lax.broadcasted_iota(jnp.int32, (nx, nx), 0) == lax.broadcasted_iota(
            jnp.int32, (nx, nx), 1
        )
        reach[...] = jnp.concatenate(
            [suffix[count - 1], jnp.where(same, 1.0, 0.0)] + [suffix[j] for j in others], axis=0
        )

        def extend(s, carry):
            received(gathered.at[s, kept], comp_recv.at[s])

            def keep(chain, value):
                at = pl.ds(pl.multiple_of((chain - 2) * nx, 128), nx)
                for i, term in enumerate(terms(value)):
                    reach_terms[i, :, at] = term

            keep(2 * s, reach[...])
            keep(2 * s + 1, exact_dot(reach[...], gathered[s, first_core]))
            reach[...] = exact_dot(reach[...], gathered[s, through])
            return carry

        lax.fori_loop(q + 1, chips, extend, 0)

    @pl.when(is_hub)
    def _():
        for p in range(count):
            for owner in (1, 0):
                j = owner * count + p
                received(carried_in.at[owner, pl.ds(0, m - owner), p], car_recv.at[j])
                total = carried[p, own_rows] if owner == 1 else None
                for d in range(owner, m):
                    value = carried_in[owner, lax.rem(k + d, m), p]
                    total = value if total is None else total + value
                carried_sum[j] = total

    spread(
        is_hub & at_end, lambda owner, p: carried_sum.at[owner * count + p],
        lambda p: own_carried.at[p, h], sum_send, lambda p: sum_recv.at[p], inner,
    )
    if count > 1:
        spread_sent(is_hub & at_end, sum_send, count - 1)

    def bring(s, rows):
        at = slice((2 * s - 2) * nx, 2 * s * nx)
        return stacked(
            jnp.concatenate([back_sum[2 * s - 2], back_sum[2 * s - 1]], axis=1),
            reach_terms[0, rows, at], reach_terms[1, rows, at], reach_terms[2, rows, at],
            dot_t,
        )

    later_chips = range(1, chips)

    @pl.when(is_hub)
    def _():
        within = {blocks - 2: carried_sum[blocks - 1]}
        for j in range(blocks - 3, -1, -1):
            within[j] = exact_dot_t(within[j + 1], coupling(j + 1)) + carried_sum[j + 1]
        for j in range(blocks - 1):
            behind_out[j] = within[j]

        behind_out[blocks - 1] = jnp.zeros((half, nx), F32)
        for s in later_chips:
            @pl.when(s > q)
            def _():
                for chain in (2 * s, 2 * s + 1):
                    received(back_in.at[chain], back_recv.at[chain])
                    total = back_in[chain, 0]
                    for d in range(1, m):
                        total += back_in[chain, d]
                    back_sum[chain - 2] = total
                more = bring(s, slice(0, 2 * nx))
                behind_out[count - 1] += more[:, :nx]
                behind_out[blocks - 1] += more[:, nx:]

    def outward(condition, order):
        spread(
            condition, lambda owner, p: behind_out.at[owner * count + p],
            lambda p: behind.at[p, h], beh_send, lambda p: beh_recv.at[p], order,
        )

    outward(is_hub, [count - 1])
    if count > 1:
        for s in later_chips:
            @pl.when(is_hub & (q > 0) & (s > q))
            def _():
                more = bring(s, slice(2 * nx, blocks * nx))
                for i, j in enumerate(others):
                    behind_out[j] += more[:, i * nx:(i + 1) * nx]

        outward(is_hub & (q > 0), reversed(range(count - 1)))
    spread_sent(is_hub & at_end, beh_send, 1)
    spread_sent(is_hub & (q > 0), beh_send, count)

    @pl.when(at_end)
    def _():
        couplings_arrive()
        for p in inner:
            arrive(own_carried, p, sum_recv.at[p])

    def finish(p, state):
        out_ref[p] = applied[p] - split_dot_t(state, following(p))

    arrive(behind, count - 1, beh_recv.at[count - 1])
    last_state = behind[count - 1].reshape(columns, nx)
    finish(count - 1, last_state)

    @pl.when(at_end)
    def _():
        state = last_state
        for p in reversed(inner):
            state = exact_dot_t(state, own_coupling[p - 1]) + own_carried[p].reshape(columns, nx)
            finish(p - 1, state)

    @pl.when(jnp.logical_not(at_end))
    def _():
        for p in reversed(range(count - 1)):
            arrive(behind, p, beh_recv.at[p])
            finish(p, behind[p].reshape(columns, nx))

    for condition, ref, semaphore in unsent:
        @pl.when(condition)
        def _():
            remote(ref, ref, semaphore, semaphore, here).wait_send()


def shards(n, m, rhs, block_inverse, entry_factor, exit_factor, previous):
    count, columns, width = rhs.shape
    nx = entry_factor.shape[2]
    padded = -(-width // 128) * 128
    if padded != width:
        extra = padded - width
        rhs = jnp.pad(rhs, ((0, 0), (0, 0), (0, extra)))
        previous = jnp.pad(previous, ((0, 0), (0, extra)))
        entry_factor = jnp.pad(entry_factor, ((0, 0), (0, extra), (0, 0)))
        exit_factor = jnp.pad(exit_factor, ((0, 0), (0, extra), (0, 0)))
        block_inverse = jnp.pad(
            block_inverse.reshape(count, width, m, width),
            ((0, 0), (0, extra), (0, 0), (0, extra)),
        ).reshape(count, padded, m * padded)
    vmem = pltpu.VMEM
    dma = pltpu.SemaphoreType.DMA
    chips = n // 2
    blocks = 2 * count
    half = columns // 2
    rest = blocks - 1
    out = pl.pallas_call(
        functools.partial(kernel, n, m),
        out_shape=pltpu.VMEM((count, columns, padded), F32),
        in_specs=[pl.BlockSpec(memory_space=pltpu.HBM)] * 5,
        out_specs=pl.BlockSpec(memory_space=pltpu.VMEM),
        scratch_shapes=[
            vmem((count, columns, padded), BF16),
            vmem(block_inverse.shape, BF16),
            vmem(entry_factor.shape, BF16),
            vmem(exit_factor.shape, BF16),
            vmem(previous.shape, BF16),
            vmem(exit_factor.shape[1:], BF16),
            vmem((count, nx + columns, nx), F32),
            vmem((2, m, count, nx + columns, nx), F32),
            vmem((columns, nx), F32),
            vmem((m, half, nx), F32),
            vmem((blocks, nx + columns, nx), F32),
            vmem((rest, nx, nx), F32),
            vmem((rest, half, nx), F32),
            vmem((3, nx, rest * nx), BF16),
            vmem((blocks * nx, nx), F32),
            vmem((3, blocks * nx, (n - 2) * nx), BF16),
            vmem((2 * nx + half, nx), F32),
            vmem((chips, 2 * nx + half, nx), F32),
            vmem((blocks, half, nx), F32),
            vmem((count, 2, half, nx), F32),
            vmem((m, count, columns, padded), BF16),
            vmem((count, columns, padded), F32),
            vmem((count, columns, nx), F32),
            vmem((2, m, count, half, nx), F32),
            vmem((blocks, half, nx), F32),
            vmem((columns, nx), F32),
            vmem((n, m, half, nx), F32),
            vmem((n - 2, half, nx), F32),
            vmem((blocks, half, nx), F32),
            vmem((count, 2, half, nx), F32),
            vmem((count, nx, nx), F32),
            vmem((count, 2, half, nx), F32),
            dma((4 + count,)),
            dma((2,)),
            dma(()), dma((blocks,)),
            dma(()), dma(()),
            dma((chips,)), dma((chips,)),
            dma((2,)), dma((count,)),
            dma((2,)), dma((m, count, 2)),
            dma(()), dma((blocks,)),
            dma(()), dma((n,)),
            dma((2,)), dma((count,)),
            dma((2,)), dma((count,)),
            dma((2,)), dma((count,)),
        ],
        compiler_params=pltpu.CompilerParams(
            collective_id=0, has_side_effects=True, vmem_limit_bytes=40 * 2**20
        ),
    )(*(
        pltpu.with_memory_space_constraint(x, pltpu.HBM)
        for x in (rhs, block_inverse, entry_factor, exit_factor, previous)
    ))
    return out[:, :, :width] if padded != width else out


def solution(mesh):
    placed = (
        P("chain", None, "col"),
        P("chain", "col", None),
        P("chain", "col", None),
        P("chain", "col", None),
        P(None, "col"),
    )
    return jax.shard_map(
        functools.partial(shards, mesh.shape["chain"], mesh.shape["col"]),
        mesh=mesh, in_specs=placed, out_specs=P("chain", None, "col"), check_vma=False,
    )
```

```python
import functools

import jax
import jax.numpy as jnp
from jax import lax
from jax.experimental import pallas as pl
from jax.experimental.pallas import tpu as pltpu
from jax.sharding import PartitionSpec as P

MESH = pl.DeviceIdType.MESH
F32 = jnp.float32
BF16 = jnp.bfloat16


def dot_t(a, b):
    return lax.dot_general(a, b, (((1,), (1,)), ((), ())), preferred_element_type=F32)


def terms(x):
    first = x.astype(BF16)
    rest = x - first.astype(F32)
    second = rest.astype(BF16)
    third = (rest - second.astype(F32)).astype(BF16)
    return first, second, third


def split_dot_t(x, low):
    rows = x.shape[0]
    product = dot_t(jnp.concatenate(terms(x), axis=0), low)
    return (product[2 * rows:] + product[rows:2 * rows]) + product[:rows]


def wide(parts):
    a1, a2, a3 = parts
    return jnp.concatenate([a3, a2, a1, a2, a1, a1], axis=1)


def tall(parts, axis):
    b1, b2, b3 = parts
    return jnp.concatenate([b1, b2, b3, b1, b2, b1], axis=axis)


def exact_dot(a, b):
    return jnp.dot(wide(terms(a)), tall(terms(b), 0), preferred_element_type=F32)


def exact_dot_t(a, b):
    return dot_t(wide(terms(a)), tall(terms(b), 1))


def prepared(ref, b):
    for i, term in enumerate(terms(b)):
        ref[i] = term


def stacked(a, b1, b2, b3, product):
    rows = a.shape[0]
    a1, a2, a3 = terms(a)
    y1 = product(jnp.concatenate([a1, a2, a3], axis=0), b1)
    y2 = product(jnp.concatenate([a1, a2], axis=0), b2)
    y3 = product(a1, b3)
    small = (y1[2 * rows:] + y2[rows:]) + y3
    return (small + (y1[rows:2 * rows] + y2[:rows])) + y1[:rows]


def plain(a, b):
    return jnp.dot(a, b, preferred_element_type=F32)


def kernel(
    n, m, rhs_hbm, binv_hbm, entry_hbm, exit_hbm, prev_hbm, out_ref,
    rhs, binv, entry, exits, prev, arriving,
    parts, parts_in, opening, opening_in, sums, prefix, prefix_add, ahead, reach, reach_terms,
    comp, gathered, states_out, states, forward, applied, carried, carried_in,
    carried_sum, offset, back_in, back_sum, behind_out, behind, own_coupling, own_carried, through_exit, near_entry, near_rhs,
    local_sem, exit_sem, part_send, part_recv, open_send, open_recv,
    comp_send, comp_recv, state_send, state_recv, fwd_send, fwd_recv,
    car_send, car_recv, back_send, back_recv, beh_send, beh_recv,
    coup_send, coup_recv, sum_send, sum_recv, near_send, near_recv,
):
    c = lax.axis_index("chain")
    k = lax.axis_index("col")
    count, columns, width = rhs.shape
    nx = entry.shape[2]
    half = columns // 2
    window = nx + half
    chips = n // 2
    q = c // 2
    core = lax.rem(c, 2)
    mids = (m // 2 - 1, m // 2)
    blocks = 2 * count
    rest = blocks - 1
    h = jnp.clip(k - mids[0], 0, 1)
    is_hub = (core == 1) & (k >= mids[0]) & (k <= mids[1])
    unsent = []

    def hub(side):
        return {"chain": 2 * q + 1, "col": mids[0] + side}

    def is_side(side):
        return (core == 1) & (k == mids[0] + side)

    low = jnp.where(k <= mids[0], 1, 0)
    far_first = (low, 1 - low)

    def remote(src, dst, send, recv, where):
        return pltpu.make_async_remote_copy(
            src_ref=src, dst_ref=dst, send_sem=send, recv_sem=recv,
            device_id=where, device_id_type=MESH,
        )

    def send(condition, *args):
        @pl.when(condition)
        def _():
            remote(*args).start()

    def sent(condition, ref, semaphore):
        unsent.append((condition, ref, semaphore))

    def received(ref, semaphore):
        remote(ref, ref, exit_sem.at[0], semaphore, here).wait_recv()

    here = {"chain": c, "col": k}
    loads = [
        pltpu.make_async_copy(exit_hbm, exits, local_sem.at[0]),
        pltpu.make_async_copy(entry_hbm, entry, local_sem.at[1]),
        pltpu.make_async_copy(rhs_hbm, rhs, local_sem.at[2]),
        pltpu.make_async_copy(prev_hbm, prev, local_sem.at[3]),
    ] + [
        pltpu.make_async_copy(binv_hbm.at[p], binv.at[p], local_sem.at[4 + p])
        for p in range(count)
    ]
    for load in loads[:4]:
        load.start()

    barrier = pltpu.get_barrier_semaphore()
    for d in range(1, m):
        for other in range(2):
            pl.semaphore_signal(
                barrier, 1, device_id={"chain": 2 * q + other, "col": lax.rem(k + d, m)},
                device_id_type=MESH,
            )
    pl.semaphore_signal(barrier, 1, device_id={"chain": 2 * q + 1 - core}, device_id_type=MESH)

    beside = c + 2 * core - 1
    has_beside = (beside >= 0) & (beside < n)

    @pl.when(has_beside)
    def _():
        pl.semaphore_signal(barrier, 1, device_id={"chain": beside}, device_id_type=MESH)

    @pl.when(is_hub)
    def _():
        for d in range(1, chips):
            pl.semaphore_signal(
                barrier, 1, device_id={"chain": 2 * lax.rem(q + d, chips) + 1},
                device_id_type=MESH,
            )

    for d in range(1, chips):
        @pl.when(is_hub & (q + d < chips))
        def _():
            for other in range(2):
                for place in range(m):
                    pl.semaphore_signal(
                        barrier, 1, device_id={"chain": 2 * (q + d) + other, "col": place},
                        device_id_type=MESH,
                    )

    @pl.when(c == n - 1)
    def _():
        arriving[...] = jnp.zeros_like(arriving)

    for load in loads[:4]:
        load.wait()
    for load in loads[4:]:
        load.start()

    @pl.when(c == 0)
    def _():
        opening[...] = jnp.dot(prev[...], exits[0], preferred_element_type=F32)

    def following(p):
        return exits[p + 1] if p + 1 < count else arriving[...]

    def part(p):
        after_p = following(p)
        source = jnp.dot(rhs[p], after_p, preferred_element_type=F32)
        parts[p, :half] = source[:half]
        parts[p, half:window] = -lax.dot_general(
            entry[p], after_p, (((0,), (0,)), ((), ())), preferred_element_type=F32
        )
        parts[p, window:] = source[half:]

    for p in range(count - 1):
        part(p)

    expected = 2 * q + 2 * m - 1 + jnp.where(has_beside, 1, 0) + jnp.where(is_hub, chips - 1, 0)
    pl.semaphore_wait(barrier, expected)

    send(c > 0, exits.at[0], arriving, exit_sem.at[0], exit_sem.at[1], {"chain": c - 1})
    sent(c > 0, arriving, exit_sem.at[0])
    for side in range(2):
        send(
            c == 0, opening.at[pl.ds(side * half, half)], opening_in.at[k],
            open_send, open_recv, hub(side),
        )
    sent(c == 0, opening, open_send)

    for p in range(count):
        if p + 1 == count:
            @pl.when(c < n - 1)
            def _():
                received(arriving, exit_sem.at[1])
            part(p)
        for side in far_first:
            rows = pl.ds(pl.multiple_of(side * half, 8), window)
            send(
                jnp.logical_not(is_side(side)), parts.at[p, rows],
                parts_in.at[core, k, p, rows], part_send,
                part_recv.at[core * count + p], hub(side),
            )
    sent(jnp.logical_not(is_hub), parts_in.at[0, pl.ds(0, 2), :, pl.ds(0, window)], part_send)
    sent(is_hub, parts_in.at[0, 0, :, pl.ds(0, window)], part_send)

    early = core == 1
    is_end = (k == 0) | (k == m - 1)
    for way, (at, to) in enumerate(((m - 2, m - 1), (1, 0))):
        give = (k == at) & early
        send(give, entry, near_entry, near_send.at[way, 0], near_recv.at[0], {"col": to})
        send(give, rhs, near_rhs, near_send.at[way, 1], near_recv.at[1], {"col": to})
        sent(give, entry, near_send.at[way, 0])
        sent(give, rhs, near_send.at[way, 1])

    added = pl.ds(0, half)
    through = pl.ds(half, nx)
    first_core = pl.ds(window, nx)
    onward = pl.ds(0, window)
    kept = pl.ds(half, 2 * nx)
    mine = pl.ds(pl.multiple_of(h * half, 8), window)
    source_rows = pl.ds(pl.multiple_of(h * window, 8), half)

    def coupling(j):
        return sums[j, half:window]

    def source(j):
        return sums[j, source_rows]

    def gather_part(j):
        owner, p = j // count, j % count
        received(parts_in.at[owner, pl.ds(0, m - owner), p, mine], part_recv.at[j])
        total = parts[p, mine] if owner == 1 else None
        for d in range(owner, m):
            value = parts_in[owner, lax.rem(k + d, m), p, mine]
            total = value if total is None else total + value
        sums[j, mine] = total

    @pl.when(is_hub)
    def _():
        gather_part(0)
        prefix[0] = coupling(0)
        prefix_add[0] = source(0)
        for j in range(1, blocks - 1):
            gather_part(j)
            both = exact_dot(
                jnp.concatenate([prefix[j - 1], prefix_add[j - 1]], axis=0), coupling(j)
            )
            prefix[j] = both[:nx]
            prefix_add[j] = both[nx:] + source(j)

        @pl.when(q == 0)
        def _():
            received(opening_in, open_recv)
            total = opening_in[0]
            for d in range(1, m):
                total += opening_in[d]
            states_out[0] = total

        last = blocks - 1
        gather_part(last)
        both = exact_dot(
            jnp.concatenate([prefix[last - 1], prefix_add[last - 1]], axis=0), coupling(last)
        )
        comp[through] = both[:nx]
        comp[added] = both[nx:] + source(last)
        comp[first_core] = prefix[count - 1]

        @pl.when(q == 0)
        def _():
            comp[added] = exact_dot(states_out[0], comp[through]) + comp[added]

    for d in range(1, chips):
        to = lax.rem(q + d, chips)
        later = {"chain": 2 * to + 1}
        send(
            is_hub & (q > 0) & (q + d < chips), comp.at[onward], gathered.at[q, onward],
            comp_send.at[to], comp_recv.at[q], later,
        )
        sent(is_hub & (q > 0) & (q + d < chips), comp.at[onward], comp_send.at[to])
        send(
            is_hub & (q == 0), comp.at[added], gathered.at[q, added], comp_send.at[to],
            comp_recv.at[q], later,
        )
        sent(is_hub & (q == 0), comp.at[added], comp_send.at[to])

    def spread(condition, source_at, target_at, sends, recv_at, order):
        for p in order:
            for i in range(m):
                to = jnp.where(h == 0, m - 1 - i, i)
                send(
                    condition, source_at(0, p), target_at(p), sends.at[0], recv_at(p),
                    {"chain": 2 * q, "col": to},
                )
                send(
                    condition & (to != k), source_at(1, p), target_at(p), sends.at[1],
                    recv_at(p), {"col": to},
                )

            @pl.when(condition)
            def _():
                target_at(p)[...] = source_at(1, p)[...]

    def spread_sent(condition, sends, amount):
        for owner, places in ((0, m), (1, m - 1)):
            sent(
                condition, carried_in.at[0, pl.ds(0, places), pl.ds(0, amount)],
                sends.at[owner],
            )

    inner = range(1, count)
    quarter = nx // 2
    at_end = q == 0
    shift = jnp.where(at_end, 1, 0)
    spread(
        is_hub,
        lambda owner, i: sums.at[
            owner * count + i + shift, pl.ds(pl.multiple_of(half + h * quarter, 8), quarter)
        ],
        lambda i: own_coupling.at[i, pl.ds(pl.multiple_of(h * quarter, 8), quarter)],
        coup_send, lambda i: coup_recv.at[i], range(count - 1),
    )
    if count > 1:
        for owner, places in ((0, m), (1, m - 1)):
            sent(
                is_hub,
                parts_in.at[0, pl.ds(0, places), pl.ds(0, count - 1), pl.ds(0, quarter)],
                coup_send.at[owner],
            )

    def couplings_arrive():
        for i in range(count - 1):
            @pl.when(is_hub)
            def _():
                received(own_coupling.at[i, pl.ds(0, quarter)], coup_recv.at[i])

            @pl.when(jnp.logical_not(is_hub))
            def _():
                received(own_coupling.at[i], coup_recv.at[i])

    @pl.when(is_hub)
    def _():
        prepared(ahead, jnp.concatenate([prefix[j] for j in range(blocks - 1)], axis=1))

        @pl.when(q > 0)
        def _():
            received(gathered.at[0, added], comp_recv.at[0])

            def fold(s, state):
                received(gathered.at[s, onward], comp_recv.at[s])
                return exact_dot(state, gathered[s, through]) + gathered[s, added]

            states_out[0] = lax.fori_loop(1, q, fold, gathered[0, added])

        spread_out = stacked(states_out[0], ahead[0], ahead[1], ahead[2], plain)
        for j in range(1, blocks):
            states_out[j] = spread_out[:, (j - 1) * nx:j * nx] + prefix_add[j - 1]

    def arrive(target, p, semaphore):
        @pl.when(is_hub)
        def _():
            received(target.at[p, 0], semaphore)

        @pl.when(jnp.logical_not(is_hub))
        def _():
            received(target.at[p], semaphore)

    spread(
        is_hub, lambda owner, p: states_out.at[owner * count + p],
        lambda p: states.at[p, h], state_send, lambda p: state_recv.at[p], range(count),
    )
    spread_sent(is_hub, state_send, count)

    for d in range(1, chips):
        to = lax.rem(q - d + chips, chips)
        send(
            is_hub & (q - d >= 0), comp.at[kept], gathered.at[q, kept],
            comp_send.at[to], comp_recv.at[q], {"chain": 2 * to + 1},
        )
        sent(is_hub & (q - d >= 0), comp.at[kept], comp_send.at[to])

    cut = -(-width // 256) * 128
    pieces = [(0, cut), (cut, width - cut)] if cut < width else [(0, width)]

    def leave(p):
        for way, step in ((0, 1), (1, -1)):
            beyond = k + step
            goes = (beyond >= 0) & (beyond < m) & jnp.logical_not(is_told(beyond))
            for piece, (start, size) in enumerate(pieces):
                part_ref = forward.at[k, p, :, pl.ds(start, size)]
                send(
                    goes, part_ref, part_ref,
                    fwd_send.at[way], fwd_recv.at[k, p, piece], {"col": beyond},
                )

    def is_told(position):
        return ((position == 0) | (position == m - 1)) & early

    for place in range(m):
        for way, last in ((0, m - 1), (1, 0)):
            if place == last:
                continue
            passed = (place + 1, m - place)[way]
            held = 1 if abs(place - last) == 1 else 0
            sent(
                (k == place) & jnp.logical_not(early), forward.at[pl.ds(0, passed)],
                fwd_send.at[way],
            )
            if passed > held:
                sent(
                    (k == place) & early, forward.at[pl.ds(0, passed - held)],
                    fwd_send.at[way],
                )

    for p in range(count):
        arrive(states, p, state_recv.at[p])
        state = states[p].reshape(columns, nx)
        forward[k, p] = (rhs[p].astype(F32) - split_dot_t(state, entry[p])).astype(BF16)
        leave(p)

    def block(j, p):
        return binv[p, :, pl.ds(pl.multiple_of(j * width, 128), width)]

    for p in range(count):
        loads[4 + p].wait()
        applied[p] = dot_t(forward[k, p], block(k, p))
    near = jnp.where(k == 0, 1, m - 2)

    @pl.when(is_end & early)
    def _():
        received(near_entry, near_recv.at[0])
        received(near_rhs, near_recv.at[1])
        for p in range(count):
            state = states[p].reshape(columns, nx)
            near_block = near_rhs[p].astype(F32) - split_dot_t(state, near_entry[p])
            applied[p] += dot_t(near_block.astype(BF16), block(near, p))

    def come(d, p, piece):
        start, size = pieces[piece]
        for way, step in ((0, 1), (1, -1)):
            j = k - step * d
            beyond = k + step
            there = (j >= 0) & (j < m)
            if d == 1:
                there &= jnp.logical_not(is_told(k))
            part_ref = forward.at[j, p, :, pl.ds(start, size)]

            @pl.when(there)
            def _():
                received(part_ref, fwd_recv.at[j, p, piece])

            if d + 1 < m:
                send(
                    there & (beyond >= 0) & (beyond < m), part_ref, part_ref,
                    fwd_send.at[way], fwd_recv.at[j, p, piece], {"col": beyond},
                )

    def multiply(d, p, start, size):
        for step in (1, -1):
            j = k - step * d
            there = (j >= 0) & (j < m)
            if d == 1:
                there &= jnp.logical_not(is_told(k))

            @pl.when(there)
            def _():
                at = pl.ds(pl.multiple_of(j * width + start, 128), size)
                applied[p] += dot_t(forward[j, p, :, pl.ds(start, size)], binv[p, :, at])

    for d in range(1, m - 1):
        for p in range(count):
            for piece in range(len(pieces)):
                come(d, p, piece)
    for d in range(1, m):
        for p in range(count):
            if d + 1 < m:
                multiply(d, p, 0, width)
            else:
                for piece, (start, size) in enumerate(pieces):
                    come(d, p, piece)
                    multiply(d, p, start, size)
            if d == m - 1:
                carried[p] = jnp.dot(
                    applied[p].astype(BF16), entry[p], preferred_element_type=F32
                )
                for side in far_first:
                    rows = pl.ds(pl.multiple_of(side * half, 8), half)
                    send(
                        jnp.logical_not(is_side(side)), carried.at[p, rows],
                        carried_in.at[core, k, p], car_send,
                        car_recv.at[core * count + p], hub(side),
                    )
    sent(jnp.logical_not(is_hub), carried_in.at[0, pl.ds(0, 2)], car_send)
    sent(is_hub, carried_in.at[0, 0], car_send)

    @pl.when(jnp.logical_not(at_end))
    def _():
        couplings_arrive()
        term = carried[count - 1]
        for p in range(count - 2, -1, -1):
            term = exact_dot_t(term, own_coupling[p]) + carried[p]
        offset[...] = term

    for t in range(chips - 1):
        for side in far_first:
            send(
                t < q, offset.at[pl.ds(pl.multiple_of(side * half, 8), half)],
                back_in.at[c, k], back_send, back_recv.at[c],
                {"chain": 2 * t + 1, "col": mids[0] + side},
            )
        sent(q == t + 1, back_in.at[pl.ds(0, t + 1), pl.ds(0, 2)], back_send)

    own_rows = pl.ds(pl.multiple_of(h * half, 8), half)

    others = [j for j in range(blocks - 1) if j != count - 1]

    @pl.when(is_hub)
    def _():
        suffix = [coupling(blocks - 1)]
        for j in range(blocks - 2, 0, -1):
            suffix.append(exact_dot(coupling(j), suffix[-1]))
        suffix = suffix[::-1]
        same = lax.broadcasted_iota(jnp.int32, (nx, nx), 0) == lax.broadcasted_iota(
            jnp.int32, (nx, nx), 1
        )
        reach[...] = jnp.concatenate(
            [suffix[count - 1], jnp.where(same, 1.0, 0.0)] + [suffix[j] for j in others], axis=0
        )

        def extend(s, carry):
            received(gathered.at[s, kept], comp_recv.at[s])

            def keep(chain, value):
                at = pl.ds(pl.multiple_of((chain - 2) * nx, 128), nx)
                for i, term in enumerate(terms(value)):
                    reach_terms[i, :, at] = term

            keep(2 * s, reach[...])
            keep(2 * s + 1, exact_dot(reach[...], gathered[s, first_core]))
            reach[...] = exact_dot(reach[...], gathered[s, through])
            return carry

        lax.fori_loop(q + 1, chips, extend, 0)

    @pl.when(is_hub)
    def _():
        for p in range(count):
            for owner in (1, 0):
                j = owner * count + p
                received(carried_in.at[owner, pl.ds(0, m - owner), p], car_recv.at[j])
                total = carried[p, own_rows] if owner == 1 else None
                for d in range(owner, m):
                    value = carried_in[owner, lax.rem(k + d, m), p]
                    total = value if total is None else total + value
                carried_sum[j] = total

    spread(
        is_hub & at_end, lambda owner, p: carried_sum.at[owner * count + p],
        lambda p: own_carried.at[p, h], sum_send, lambda p: sum_recv.at[p], inner,
    )
    if count > 1:
        spread_sent(is_hub & at_end, sum_send, count - 1)

    def bring(s, rows):
        at = slice((2 * s - 2) * nx, 2 * s * nx)
        return stacked(
            jnp.concatenate([back_sum[2 * s - 2], back_sum[2 * s - 1]], axis=1),
            reach_terms[0, rows, at], reach_terms[1, rows, at], reach_terms[2, rows, at],
            dot_t,
        )

    later_chips = range(1, chips)

    @pl.when(is_hub)
    def _():
        within = {blocks - 2: carried_sum[blocks - 1]}
        for j in range(blocks - 3, -1, -1):
            within[j] = exact_dot_t(within[j + 1], coupling(j + 1)) + carried_sum[j + 1]
        for j in range(blocks - 1):
            behind_out[j] = within[j]

        behind_out[blocks - 1] = jnp.zeros((half, nx), F32)
        for s in later_chips:
            @pl.when(s > q)
            def _():
                for chain in (2 * s, 2 * s + 1):
                    received(back_in.at[chain], back_recv.at[chain])
                    total = back_in[chain, 0]
                    for d in range(1, m):
                        total += back_in[chain, d]
                    back_sum[chain - 2] = total
                more = bring(s, slice(0, 2 * nx))
                behind_out[count - 1] += more[:, :nx]
                behind_out[blocks - 1] += more[:, nx:]

    def outward(condition, order):
        spread(
            condition, lambda owner, p: behind_out.at[owner * count + p],
            lambda p: behind.at[p, h], beh_send, lambda p: beh_recv.at[p], order,
        )

    outward(is_hub, [count - 1])
    if count > 1:
        for s in later_chips:
            @pl.when(is_hub & (q > 0) & (s > q))
            def _():
                more = bring(s, slice(2 * nx, blocks * nx))
                for i, j in enumerate(others):
                    behind_out[j] += more[:, i * nx:(i + 1) * nx]

        outward(is_hub & (q > 0), reversed(range(count - 1)))
    spread_sent(is_hub & at_end, beh_send, 1)
    spread_sent(is_hub & (q > 0), beh_send, count)

    @pl.when(at_end)
    def _():
        couplings_arrive()
        for p in inner:
            arrive(own_carried, p, sum_recv.at[p])
        factor, remainder = None, None
        for p in range(count - 2, -1, -1):
            sum_here = own_carried[p + 1].reshape(columns, nx)
            if factor is None:
                factor, remainder = own_coupling[p], sum_here
            else:
                factor = exact_dot(own_coupling[p], factor)
                remainder = exact_dot_t(remainder, own_coupling[p]) + sum_here
            low = following(p)
            c1, c2, c3 = terms(factor)
            row = (plain(low, c3) + plain(low, c2)) + plain(low, c1)
            for i, term in enumerate(terms(row)):
                through_exit[p, i] = term
            applied[p] = applied[p] - split_dot_t(remainder, low)

    def finish(p, state):
        out_ref[p] = applied[p] - split_dot_t(state, following(p))

    arrive(behind, count - 1, beh_recv.at[count - 1])
    last_state = behind[count - 1].reshape(columns, nx)

    @pl.when(at_end)
    def _():
        for p in range(count - 1):
            out_ref[p] = applied[p] - stacked(
                last_state, through_exit[p, 0], through_exit[p, 1], through_exit[p, 2], dot_t
            )
        finish(count - 1, last_state)

    @pl.when(jnp.logical_not(at_end))
    def _():
        finish(count - 1, last_state)
        for p in reversed(range(count - 1)):
            arrive(behind, p, beh_recv.at[p])
            finish(p, behind[p].reshape(columns, nx))

    for condition, ref, semaphore in unsent:
        @pl.when(condition)
        def _():
            remote(ref, ref, semaphore, semaphore, here).wait_send()


def shards(n, m, rhs, block_inverse, entry_factor, exit_factor, previous):
    count, columns, width = rhs.shape
    nx = entry_factor.shape[2]
    padded = -(-width // 128) * 128
    if padded != width:
        extra = padded - width
        rhs = jnp.pad(rhs, ((0, 0), (0, 0), (0, extra)))
        previous = jnp.pad(previous, ((0, 0), (0, extra)))
        entry_factor = jnp.pad(entry_factor, ((0, 0), (0, extra), (0, 0)))
        exit_factor = jnp.pad(exit_factor, ((0, 0), (0, extra), (0, 0)))
        block_inverse = jnp.pad(
            block_inverse.reshape(count, width, m, width),
            ((0, 0), (0, extra), (0, 0), (0, extra)),
        ).reshape(count, padded, m * padded)
    vmem = pltpu.VMEM
    dma = pltpu.SemaphoreType.DMA
    chips = n // 2
    blocks = 2 * count
    half = columns // 2
    rest = blocks - 1
    out = pl.pallas_call(
        functools.partial(kernel, n, m),
        out_shape=pltpu.VMEM((count, columns, padded), F32),
        in_specs=[pl.BlockSpec(memory_space=pltpu.HBM)] * 5,
        out_specs=pl.BlockSpec(memory_space=pltpu.VMEM),
        scratch_shapes=[
            vmem((count, columns, padded), BF16),
            vmem(block_inverse.shape, BF16),
            vmem(entry_factor.shape, BF16),
            vmem(exit_factor.shape, BF16),
            vmem(previous.shape, BF16),
            vmem(exit_factor.shape[1:], BF16),
            vmem((count, nx + columns, nx), F32),
            vmem((2, m, count, nx + columns, nx), F32),
            vmem((columns, nx), F32),
            vmem((m, half, nx), F32),
            vmem((blocks, nx + columns, nx), F32),
            vmem((rest, nx, nx), F32),
            vmem((rest, half, nx), F32),
            vmem((3, nx, rest * nx), BF16),
            vmem((blocks * nx, nx), F32),
            vmem((3, blocks * nx, (n - 2) * nx), BF16),
            vmem((2 * nx + half, nx), F32),
            vmem((chips, 2 * nx + half, nx), F32),
            vmem((blocks, half, nx), F32),
            vmem((count, 2, half, nx), F32),
            vmem((m, count, columns, padded), BF16),
            vmem((count, columns, padded), F32),
            vmem((count, columns, nx), F32),
            vmem((2, m, count, half, nx), F32),
            vmem((blocks, half, nx), F32),
            vmem((columns, nx), F32),
            vmem((n, m, half, nx), F32),
            vmem((n - 2, half, nx), F32),
            vmem((blocks, half, nx), F32),
            vmem((count, 2, half, nx), F32),
            vmem((count, nx, nx), F32),
            vmem((count, 2, half, nx), F32),
            vmem((count, 3, padded, nx), BF16),
            vmem(entry_factor.shape, BF16),
            vmem((count, columns, padded), BF16),
            dma((4 + count,)),
            dma((2,)),
            dma(()), dma((blocks,)),
            dma(()), dma(()),
            dma((chips,)), dma((chips,)),
            dma((2,)), dma((count,)),
            dma((2,)), dma((m, count, 2)),
            dma(()), dma((blocks,)),
            dma(()), dma((n,)),
            dma((2,)), dma((count,)),
            dma((2,)), dma((count,)),
            dma((2,)), dma((count,)),
            dma((2, 2)), dma((2,)),
        ],
        compiler_params=pltpu.CompilerParams(
            collective_id=0, has_side_effects=True, vmem_limit_bytes=40 * 2**20
        ),
    )(*(
        pltpu.with_memory_space_constraint(x, pltpu.HBM)
        for x in (rhs, block_inverse, entry_factor, exit_factor, previous)
    ))
    return out[:, :, :width] if padded != width else out


def solution(mesh):
    placed = (
        P("chain", None, "col"),
        P("chain", "col", None),
        P("chain", "col", None),
        P("chain", "col", None),
        P(None, "col"),
    )
    return jax.shard_map(
        functools.partial(shards, mesh.shape["chain"], mesh.shape["col"]),
        mesh=mesh, in_specs=placed, out_specs=P("chain", None, "col"), check_vma=False,
    )
```

```python
import functools

import jax
import jax.numpy as jnp
from jax import lax
from jax.experimental import pallas as pl
from jax.experimental.pallas import tpu as pltpu
from jax.sharding import PartitionSpec as P

MESH = pl.DeviceIdType.MESH
F32 = jnp.float32
BF16 = jnp.bfloat16


def dot_t(a, b):
    return lax.dot_general(a, b, (((1,), (1,)), ((), ())), preferred_element_type=F32)


def terms(x):
    first = x.astype(BF16)
    rest = x - first.astype(F32)
    second = rest.astype(BF16)
    third = (rest - second.astype(F32)).astype(BF16)
    return first, second, third


def split_dot_t(x, low):
    rows = x.shape[0]
    product = dot_t(jnp.concatenate(terms(x), axis=0), low)
    return (product[2 * rows:] + product[rows:2 * rows]) + product[:rows]


def wide(parts):
    a1, a2, a3 = parts
    return jnp.concatenate([a3, a2, a1, a2, a1, a1], axis=1)


def tall(parts, axis):
    b1, b2, b3 = parts
    return jnp.concatenate([b1, b2, b3, b1, b2, b1], axis=axis)


def exact_dot(a, b):
    return jnp.dot(wide(terms(a)), tall(terms(b), 0), preferred_element_type=F32)


def exact_dot_t(a, b):
    return dot_t(wide(terms(a)), tall(terms(b), 1))


def prepared(ref, b):
    for i, term in enumerate(terms(b)):
        ref[i] = term


def stacked(a, b1, b2, b3, product):
    rows = a.shape[0]
    a1, a2, a3 = terms(a)
    y1 = product(jnp.concatenate([a1, a2, a3], axis=0), b1)
    y2 = product(jnp.concatenate([a1, a2], axis=0), b2)
    y3 = product(a1, b3)
    small = (y1[2 * rows:] + y2[rows:]) + y3
    return (small + (y1[rows:2 * rows] + y2[:rows])) + y1[:rows]


def plain(a, b):
    return jnp.dot(a, b, preferred_element_type=F32)


def kernel(
    n, m, rhs_hbm, binv_hbm, entry_hbm, exit_hbm, prev_hbm, out_ref,
    rhs, binv, entry, exits, prev, arriving,
    parts, parts_in, opening, opening_in, sums, prefix, prefix_add, ahead, reach, reach_terms,
    comp, gathered, states_out, states, forward, applied, carried, carried_in,
    carried_sum, offset, back_in, back_sum, behind_out, behind, own_coupling, own_carried, through_exit, near_entry, near_rhs,
    local_sem, exit_sem, part_send, part_recv, open_send, open_recv,
    comp_send, comp_recv, state_send, state_recv, fwd_send, fwd_recv,
    car_send, car_recv, back_send, back_recv, beh_send, beh_recv,
    coup_send, coup_recv, sum_send, sum_recv, near_send, near_recv,
):
    c = lax.axis_index("chain")
    k = lax.axis_index("col")
    count, columns, width = rhs.shape
    nx = entry.shape[2]
    half = columns // 2
    window = nx + half
    chips = n // 2
    q = c // 2
    core = lax.rem(c, 2)
    mids = (m // 2 - 1, m // 2)
    blocks = 2 * count
    rest = blocks - 1
    h = jnp.clip(k - mids[0], 0, 1)
    is_hub = (core == 1) & (k >= mids[0]) & (k <= mids[1])
    unsent = []

    def hub(side):
        return {"chain": 2 * q + 1, "col": mids[0] + side}

    def is_side(side):
        return (core == 1) & (k == mids[0] + side)

    low = jnp.where(k <= mids[0], 1, 0)
    far_first = (low, 1 - low)

    def remote(src, dst, send, recv, where):
        return pltpu.make_async_remote_copy(
            src_ref=src, dst_ref=dst, send_sem=send, recv_sem=recv,
            device_id=where, device_id_type=MESH,
        )

    def send(condition, *args):
        @pl.when(condition)
        def _():
            remote(*args).start()

    def sent(condition, ref, semaphore):
        unsent.append((condition, ref, semaphore))

    def received(ref, semaphore):
        remote(ref, ref, exit_sem.at[0], semaphore, here).wait_recv()

    here = {"chain": c, "col": k}
    loads = [
        pltpu.make_async_copy(exit_hbm, exits, local_sem.at[0]),
        pltpu.make_async_copy(entry_hbm, entry, local_sem.at[1]),
        pltpu.make_async_copy(rhs_hbm, rhs, local_sem.at[2]),
        pltpu.make_async_copy(prev_hbm, prev, local_sem.at[3]),
    ] + [
        pltpu.make_async_copy(binv_hbm.at[p], binv.at[p], local_sem.at[4 + p])
        for p in range(count)
    ]
    for load in loads[:4]:
        load.start()

    barrier = pltpu.get_barrier_semaphore()
    for d in range(1, m):
        for other in range(2):
            pl.semaphore_signal(
                barrier, 1, device_id={"chain": 2 * q + other, "col": lax.rem(k + d, m)},
                device_id_type=MESH,
            )
    pl.semaphore_signal(barrier, 1, device_id={"chain": 2 * q + 1 - core}, device_id_type=MESH)

    beside = c + 2 * core - 1
    has_beside = (beside >= 0) & (beside < n)

    @pl.when(has_beside)
    def _():
        pl.semaphore_signal(barrier, 1, device_id={"chain": beside}, device_id_type=MESH)

    @pl.when(is_hub)
    def _():
        for d in range(1, chips):
            pl.semaphore_signal(
                barrier, 1, device_id={"chain": 2 * lax.rem(q + d, chips) + 1},
                device_id_type=MESH,
            )

    for d in range(1, chips):
        @pl.when(is_hub & (q + d < chips))
        def _():
            for other in range(2):
                for place in range(m):
                    pl.semaphore_signal(
                        barrier, 1, device_id={"chain": 2 * (q + d) + other, "col": place},
                        device_id_type=MESH,
                    )

    @pl.when(c == n - 1)
    def _():
        arriving[...] = jnp.zeros_like(arriving)

    for load in loads[:4]:
        load.wait()
    for load in loads[4:]:
        load.start()

    @pl.when(c == 0)
    def _():
        opening[...] = jnp.dot(prev[...], exits[0], preferred_element_type=F32)

    def following(p):
        return exits[p + 1] if p + 1 < count else arriving[...]

    def part(p):
        after_p = following(p)
        source = jnp.dot(rhs[p], after_p, preferred_element_type=F32)
        parts[p, :half] = source[:half]
        parts[p, half:window] = -lax.dot_general(
            entry[p], after_p, (((0,), (0,)), ((), ())), preferred_element_type=F32
        )
        parts[p, window:] = source[half:]

    for p in range(count - 1):
        part(p)

    expected = 2 * q + 2 * m - 1 + jnp.where(has_beside, 1, 0) + jnp.where(is_hub, chips - 1, 0)
    pl.semaphore_wait(barrier, expected)

    send(c > 0, exits.at[0], arriving, exit_sem.at[0], exit_sem.at[1], {"chain": c - 1})
    sent(c > 0, arriving, exit_sem.at[0])
    for side in range(2):
        send(
            c == 0, opening.at[pl.ds(side * half, half)], opening_in.at[k],
            open_send, open_recv, hub(side),
        )
    sent(c == 0, opening, open_send)

    for p in range(count):
        if p + 1 == count:
            @pl.when(c < n - 1)
            def _():
                received(arriving, exit_sem.at[1])
            part(p)
        for side in far_first:
            rows = pl.ds(pl.multiple_of(side * half, 8), window)
            send(
                jnp.logical_not(is_side(side)), parts.at[p, rows],
                parts_in.at[core, k, p, rows], part_send,
                part_recv.at[core * count + p], hub(side),
            )
    sent(jnp.logical_not(is_hub), parts_in.at[0, pl.ds(0, 2), :, pl.ds(0, window)], part_send)
    sent(is_hub, parts_in.at[0, 0, :, pl.ds(0, window)], part_send)

    early = core == 1
    is_end = (k == 0) | (k == m - 1)
    for way, (at, to) in enumerate(((m - 2, m - 1), (1, 0))):
        give = (k == at) & early
        send(give, entry, near_entry, near_send.at[way, 0], near_recv.at[0], {"col": to})
        send(give, rhs, near_rhs, near_send.at[way, 1], near_recv.at[1], {"col": to})
        sent(give, entry, near_send.at[way, 0])
        sent(give, rhs, near_send.at[way, 1])

    added = pl.ds(0, half)
    through = pl.ds(half, nx)
    first_core = pl.ds(window, nx)
    onward = pl.ds(0, window)
    kept = pl.ds(half, 2 * nx)
    mine = pl.ds(pl.multiple_of(h * half, 8), window)
    source_rows = pl.ds(pl.multiple_of(h * window, 8), half)

    def coupling(j):
        return sums[j, half:window]

    def source(j):
        return sums[j, source_rows]

    def gather_part(j):
        owner, p = j // count, j % count
        received(parts_in.at[owner, pl.ds(0, m - owner), p, mine], part_recv.at[j])
        total = parts[p, mine] if owner == 1 else None
        for d in range(owner, m):
            value = parts_in[owner, lax.rem(k + d, m), p, mine]
            total = value if total is None else total + value
        sums[j, mine] = total

    @pl.when(is_hub)
    def _():
        gather_part(0)
        prefix[0] = coupling(0)
        prefix_add[0] = source(0)
        for j in range(1, blocks - 1):
            gather_part(j)
            both = exact_dot(
                jnp.concatenate([prefix[j - 1], prefix_add[j - 1]], axis=0), coupling(j)
            )
            prefix[j] = both[:nx]
            prefix_add[j] = both[nx:] + source(j)

        @pl.when(q == 0)
        def _():
            received(opening_in, open_recv)
            total = opening_in[0]
            for d in range(1, m):
                total += opening_in[d]
            states_out[0] = total

        last = blocks - 1
        gather_part(last)
        both = exact_dot(
            jnp.concatenate([prefix[last - 1], prefix_add[last - 1]], axis=0), coupling(last)
        )
        comp[through] = both[:nx]
        comp[added] = both[nx:] + source(last)
        comp[first_core] = prefix[count - 1]

        @pl.when(q == 0)
        def _():
            comp[added] = exact_dot(states_out[0], comp[through]) + comp[added]

    for d in range(1, chips):
        to = lax.rem(q + d, chips)
        later = {"chain": 2 * to + 1}
        send(
            is_hub & (q > 0) & (q + d < chips), comp.at[onward], gathered.at[q, onward],
            comp_send.at[to], comp_recv.at[q], later,
        )
        sent(is_hub & (q > 0) & (q + d < chips), comp.at[onward], comp_send.at[to])
        send(
            is_hub & (q == 0), comp.at[added], gathered.at[q, added], comp_send.at[to],
            comp_recv.at[q], later,
        )
        sent(is_hub & (q == 0), comp.at[added], comp_send.at[to])

    def spread(condition, source_at, target_at, sends, recv_at, order):
        for p in order:
            for i in range(m):
                to = jnp.where(h == 0, m - 1 - i, i)
                send(
                    condition, source_at(0, p), target_at(p), sends.at[0], recv_at(p),
                    {"chain": 2 * q, "col": to},
                )
                send(
                    condition & (to != k), source_at(1, p), target_at(p), sends.at[1],
                    recv_at(p), {"col": to},
                )

            @pl.when(condition)
            def _():
                target_at(p)[...] = source_at(1, p)[...]

    def spread_sent(condition, sends, amount):
        for owner, places in ((0, m), (1, m - 1)):
            sent(
                condition, carried_in.at[0, pl.ds(0, places), pl.ds(0, amount)],
                sends.at[owner],
            )

    inner = range(1, count)
    quarter = nx // 2
    at_end = q == 0
    shift = jnp.where(at_end, 1, 0)
    spread(
        is_hub,
        lambda owner, i: sums.at[
            owner * count + i + shift, pl.ds(pl.multiple_of(half + h * quarter, 8), quarter)
        ],
        lambda i: own_coupling.at[i, pl.ds(pl.multiple_of(h * quarter, 8), quarter)],
        coup_send, lambda i: coup_recv.at[i], range(count - 1),
    )
    if count > 1:
        for owner, places in ((0, m), (1, m - 1)):
            sent(
                is_hub,
                parts_in.at[0, pl.ds(0, places), pl.ds(0, count - 1), pl.ds(0, quarter)],
                coup_send.at[owner],
            )

    def couplings_arrive():
        for i in range(count - 1):
            @pl.when(is_hub)
            def _():
                received(own_coupling.at[i, pl.ds(0, quarter)], coup_recv.at[i])

            @pl.when(jnp.logical_not(is_hub))
            def _():
                received(own_coupling.at[i], coup_recv.at[i])

    @pl.when(is_hub)
    def _():
        prepared(ahead, jnp.concatenate([prefix[j] for j in range(blocks - 1)], axis=1))

        @pl.when(q > 0)
        def _():
            received(gathered.at[0, added], comp_recv.at[0])

            def fold(s, state):
                received(gathered.at[s, onward], comp_recv.at[s])
                return exact_dot(state, gathered[s, through]) + gathered[s, added]

            states_out[0] = lax.fori_loop(1, q, fold, gathered[0, added])

        spread_out = stacked(states_out[0], ahead[0], ahead[1], ahead[2], plain)
        for j in range(1, blocks):
            states_out[j] = spread_out[:, (j - 1) * nx:j * nx] + prefix_add[j - 1]

    def arrive(target, p, semaphore):
        @pl.when(is_hub)
        def _():
            received(target.at[p, 0], semaphore)

        @pl.when(jnp.logical_not(is_hub))
        def _():
            received(target.at[p], semaphore)

    spread(
        is_hub, lambda owner, p: states_out.at[owner * count + p],
        lambda p: states.at[p, h], state_send, lambda p: state_recv.at[p], range(count),
    )
    spread_sent(is_hub, state_send, count)

    for d in range(1, chips):
        to = lax.rem(q - d + chips, chips)
        send(
            is_hub & (q - d >= 0), comp.at[kept], gathered.at[q, kept],
            comp_send.at[to], comp_recv.at[q], {"chain": 2 * to + 1},
        )
        sent(is_hub & (q - d >= 0), comp.at[kept], comp_send.at[to])

    cut = -(-width // 256) * 128
    pieces = [(0, cut), (cut, width - cut)] if cut < width else [(0, width)]

    def leave(p):
        for way, step in ((0, 1), (1, -1)):
            beyond = k + step
            goes = (beyond >= 0) & (beyond < m) & jnp.logical_not(is_told(beyond))
            for piece, (start, size) in enumerate(pieces):
                part_ref = forward.at[k, p, :, pl.ds(start, size)]
                send(
                    goes, part_ref, part_ref,
                    fwd_send.at[way], fwd_recv.at[k, p, piece], {"col": beyond},
                )

    def is_told(position):
        return ((position == 0) | (position == m - 1)) & early

    for place in range(m):
        for way, last in ((0, m - 1), (1, 0)):
            if place == last:
                continue
            passed = (place + 1, m - place)[way]
            held = 1 if abs(place - last) == 1 else 0
            sent(
                (k == place) & jnp.logical_not(early), forward.at[pl.ds(0, passed)],
                fwd_send.at[way],
            )
            if passed > held:
                sent(
                    (k == place) & early, forward.at[pl.ds(0, passed - held)],
                    fwd_send.at[way],
                )

    for p in range(count):
        arrive(states, p, state_recv.at[p])
        state = states[p].reshape(columns, nx)
        forward[k, p] = (rhs[p].astype(F32) - split_dot_t(state, entry[p])).astype(BF16)
        leave(p)

    def block(j, p):
        return binv[p, :, pl.ds(pl.multiple_of(j * width, 128), width)]

    for p in range(count):
        loads[4 + p].wait()
        applied[p] = dot_t(forward[k, p], block(k, p))
    near = jnp.where(k == 0, 1, m - 2)

    @pl.when(is_end & early)
    def _():
        received(near_entry, near_recv.at[0])
        received(near_rhs, near_recv.at[1])
        for p in range(count):
            state = states[p].reshape(columns, nx)
            near_block = near_rhs[p].astype(F32) - split_dot_t(state, near_entry[p])
            applied[p] += dot_t(near_block.astype(BF16), block(near, p))

    def come(d, p, piece):
        start, size = pieces[piece]
        for way, step in ((0, 1), (1, -1)):
            j = k - step * d
            beyond = k + step
            there = (j >= 0) & (j < m)
            if d == 1:
                there &= jnp.logical_not(is_told(k))
            part_ref = forward.at[j, p, :, pl.ds(start, size)]

            @pl.when(there)
            def _():
                received(part_ref, fwd_recv.at[j, p, piece])

            if d + 1 < m:
                send(
                    there & (beyond >= 0) & (beyond < m), part_ref, part_ref,
                    fwd_send.at[way], fwd_recv.at[j, p, piece], {"col": beyond},
                )

    def multiply(d, p, start, size):
        for step in (1, -1):
            j = k - step * d
            there = (j >= 0) & (j < m)
            if d == 1:
                there &= jnp.logical_not(is_told(k))

            @pl.when(there)
            def _():
                at = pl.ds(pl.multiple_of(j * width + start, 128), size)
                applied[p] += dot_t(forward[j, p, :, pl.ds(start, size)], binv[p, :, at])

    for d in range(1, m - 1):
        for p in range(count):
            for piece in range(len(pieces)):
                come(d, p, piece)
    for d in range(1, m):
        for p in range(count):
            if d + 1 < m:
                multiply(d, p, 0, width)
            else:
                for piece, (start, size) in enumerate(pieces):
                    come(d, p, piece)
                    multiply(d, p, start, size)
            if d == m - 1:
                carried[p] = jnp.dot(
                    applied[p].astype(BF16), entry[p], preferred_element_type=F32
                )

    sent(jnp.logical_not(is_hub), carried_in.at[0, pl.ds(0, 2)], car_send)
    sent(is_hub, carried_in.at[0, 0], car_send)

    @pl.when(jnp.logical_not(at_end))
    def _():
        couplings_arrive()
        term = carried[count - 1]
        for p in range(count - 2, -1, -1):
            term = exact_dot_t(term, own_coupling[p]) + carried[p]
        offset[...] = term

    for t in range(chips - 1):
        for side in far_first:
            send(
                t < q, offset.at[pl.ds(pl.multiple_of(side * half, 8), half)],
                back_in.at[c, k], back_send, back_recv.at[q],
                {"chain": 2 * t + 1, "col": mids[0] + side},
            )
        sent(q == t + 1, back_in.at[pl.ds(0, t + 1), pl.ds(0, 2)], back_send)

    for p in range(count):
        for side in far_first:
            rows = pl.ds(pl.multiple_of(side * half, 8), half)
            send(
                jnp.logical_not(is_side(side)), carried.at[p, rows], carried_in.at[core, k, p],
                car_send, car_recv.at[core * count + p], hub(side),
            )

    own_rows = pl.ds(pl.multiple_of(h * half, 8), half)

    others = [j for j in range(blocks - 1) if j != count - 1]

    @pl.when(is_hub)
    def _():
        suffix = [coupling(blocks - 1)]
        for j in range(blocks - 2, 0, -1):
            suffix.append(exact_dot(coupling(j), suffix[-1]))
        suffix = suffix[::-1]
        same = lax.broadcasted_iota(jnp.int32, (nx, nx), 0) == lax.broadcasted_iota(
            jnp.int32, (nx, nx), 1
        )
        reach[...] = jnp.concatenate(
            [suffix[count - 1], jnp.where(same, 1.0, 0.0)] + [suffix[j] for j in others], axis=0
        )

        def extend(s, carry):
            received(gathered.at[s, kept], comp_recv.at[s])

            def keep(chain, value):
                at = pl.ds(pl.multiple_of((chain - 2) * nx, 128), nx)
                for i, term in enumerate(terms(value)):
                    reach_terms[i, :, at] = term

            keep(2 * s, reach[...])
            keep(2 * s + 1, exact_dot(reach[...], gathered[s, first_core]))
            reach[...] = exact_dot(reach[...], gathered[s, through])
            return carry

        lax.fori_loop(q + 1, chips, extend, 0)

    @pl.when(is_hub)
    def _():
        for p in range(count):
            for owner in (1, 0):
                j = owner * count + p
                received(carried_in.at[owner, pl.ds(0, m - owner), p], car_recv.at[j])
                total = carried[p, own_rows] if owner == 1 else None
                for d in range(owner, m):
                    value = carried_in[owner, lax.rem(k + d, m), p]
                    total = value if total is None else total + value
                carried_sum[j] = total

    spread(
        is_hub & at_end, lambda owner, p: carried_sum.at[owner * count + p],
        lambda p: own_carried.at[p, h], sum_send, lambda p: sum_recv.at[p], inner,
    )
    if count > 1:
        spread_sent(is_hub & at_end, sum_send, count - 1)

    def bring(s, rows):
        at = slice((2 * s - 2) * nx, 2 * s * nx)
        return stacked(
            jnp.concatenate([back_sum[2 * s - 2], back_sum[2 * s - 1]], axis=1),
            reach_terms[0, rows, at], reach_terms[1, rows, at], reach_terms[2, rows, at],
            dot_t,
        )

    later_chips = range(1, chips)

    @pl.when(is_hub)
    def _():
        within = {blocks - 2: carried_sum[blocks - 1]}
        for j in range(blocks - 3, -1, -1):
            within[j] = exact_dot_t(within[j + 1], coupling(j + 1)) + carried_sum[j + 1]
        for j in range(blocks - 1):
            behind_out[j] = within[j]

        behind_out[blocks - 1] = jnp.zeros((half, nx), F32)
        for s in later_chips:
            @pl.when(s > q)
            def _():
                received(back_in.at[pl.ds(2 * s, 2)], back_recv.at[s])
                for chain in (2 * s, 2 * s + 1):
                    total = back_in[chain, 0]
                    for d in range(1, m):
                        total += back_in[chain, d]
                    back_sum[chain - 2] = total
                more = bring(s, slice(0, 2 * nx))
                behind_out[count - 1] += more[:, :nx]
                behind_out[blocks - 1] += more[:, nx:]

    def outward(condition, order):
        spread(
            condition, lambda owner, p: behind_out.at[owner * count + p],
            lambda p: behind.at[p, h], beh_send, lambda p: beh_recv.at[p], order,
        )

    outward(is_hub, [count - 1])
    if count > 1:
        for s in later_chips:
            @pl.when(is_hub & (q > 0) & (s > q))
            def _():
                more = bring(s, slice(2 * nx, blocks * nx))
                for i, j in enumerate(others):
                    behind_out[j] += more[:, i * nx:(i + 1) * nx]

        outward(is_hub & (q > 0), reversed(range(count - 1)))
    spread_sent(is_hub & at_end, beh_send, 1)
    spread_sent(is_hub & (q > 0), beh_send, count)

    @pl.when(at_end)
    def _():
        couplings_arrive()
        for p in inner:
            arrive(own_carried, p, sum_recv.at[p])
        factor, remainder = None, None
        for p in range(count - 2, -1, -1):
            sum_here = own_carried[p + 1].reshape(columns, nx)
            if factor is None:
                factor, remainder = own_coupling[p], sum_here
            else:
                factor = exact_dot(own_coupling[p], factor)
                remainder = exact_dot_t(remainder, own_coupling[p]) + sum_here
            low = following(p)
            c1, c2, c3 = terms(factor)
            row = (plain(low, c3) + plain(low, c2)) + plain(low, c1)
            for i, term in enumerate(terms(row)):
                through_exit[p, i] = term
            applied[p] = applied[p] - split_dot_t(remainder, low)

    def finish(p, state):
        out_ref[p] = applied[p] - split_dot_t(state, following(p))

    arrive(behind, count - 1, beh_recv.at[count - 1])
    last_state = behind[count - 1].reshape(columns, nx)

    @pl.when(at_end)
    def _():
        for p in range(count - 1):
            out_ref[p] = applied[p] - stacked(
                last_state, through_exit[p, 0], through_exit[p, 1], through_exit[p, 2], dot_t
            )
        finish(count - 1, last_state)

    @pl.when(jnp.logical_not(at_end))
    def _():
        finish(count - 1, last_state)
        for p in reversed(range(count - 1)):
            arrive(behind, p, beh_recv.at[p])
            finish(p, behind[p].reshape(columns, nx))

    for condition, ref, semaphore in unsent:
        @pl.when(condition)
        def _():
            remote(ref, ref, semaphore, semaphore, here).wait_send()


def shards(n, m, rhs, block_inverse, entry_factor, exit_factor, previous):
    count, columns, width = rhs.shape
    nx = entry_factor.shape[2]
    padded = -(-width // 128) * 128
    if padded != width:
        extra = padded - width
        rhs = jnp.pad(rhs, ((0, 0), (0, 0), (0, extra)))
        previous = jnp.pad(previous, ((0, 0), (0, extra)))
        entry_factor = jnp.pad(entry_factor, ((0, 0), (0, extra), (0, 0)))
        exit_factor = jnp.pad(exit_factor, ((0, 0), (0, extra), (0, 0)))
        block_inverse = jnp.pad(
            block_inverse.reshape(count, width, m, width),
            ((0, 0), (0, extra), (0, 0), (0, extra)),
        ).reshape(count, padded, m * padded)
    vmem = pltpu.VMEM
    dma = pltpu.SemaphoreType.DMA
    chips = n // 2
    blocks = 2 * count
    half = columns // 2
    rest = blocks - 1
    out = pl.pallas_call(
        functools.partial(kernel, n, m),
        out_shape=pltpu.VMEM((count, columns, padded), F32),
        in_specs=[pl.BlockSpec(memory_space=pltpu.HBM)] * 5,
        out_specs=pl.BlockSpec(memory_space=pltpu.VMEM),
        scratch_shapes=[
            vmem((count, columns, padded), BF16),
            vmem(block_inverse.shape, BF16),
            vmem(entry_factor.shape, BF16),
            vmem(exit_factor.shape, BF16),
            vmem(previous.shape, BF16),
            vmem(exit_factor.shape[1:], BF16),
            vmem((count, nx + columns, nx), F32),
            vmem((2, m, count, nx + columns, nx), F32),
            vmem((columns, nx), F32),
            vmem((m, half, nx), F32),
            vmem((blocks, nx + columns, nx), F32),
            vmem((rest, nx, nx), F32),
            vmem((rest, half, nx), F32),
            vmem((3, nx, rest * nx), BF16),
            vmem((blocks * nx, nx), F32),
            vmem((3, blocks * nx, (n - 2) * nx), BF16),
            vmem((2 * nx + half, nx), F32),
            vmem((chips, 2 * nx + half, nx), F32),
            vmem((blocks, half, nx), F32),
            vmem((count, 2, half, nx), F32),
            vmem((m, count, columns, padded), BF16),
            vmem((count, columns, padded), F32),
            vmem((count, columns, nx), F32),
            vmem((2, m, count, half, nx), F32),
            vmem((blocks, half, nx), F32),
            vmem((columns, nx), F32),
            vmem((n, m, half, nx), F32),
            vmem((n - 2, half, nx), F32),
            vmem((blocks, half, nx), F32),
            vmem((count, 2, half, nx), F32),
            vmem((count, nx, nx), F32),
            vmem((count, 2, half, nx), F32),
            vmem((count, 3, padded, nx), BF16),
            vmem(entry_factor.shape, BF16),
            vmem((count, columns, padded), BF16),
            dma((4 + count,)),
            dma((2,)),
            dma(()), dma((blocks,)),
            dma(()), dma(()),
            dma((chips,)), dma((chips,)),
            dma((2,)), dma((count,)),
            dma((2,)), dma((m, count, 2)),
            dma(()), dma((blocks,)),
            dma(()), dma((chips,)),
            dma((2,)), dma((count,)),
            dma((2,)), dma((count,)),
            dma((2,)), dma((count,)),
            dma((2, 2)), dma((2,)),
        ],
        compiler_params=pltpu.CompilerParams(
            collective_id=0, has_side_effects=True, vmem_limit_bytes=40 * 2**20
        ),
    )(*(
        pltpu.with_memory_space_constraint(x, pltpu.HBM)
        for x in (rhs, block_inverse, entry_factor, exit_factor, previous)
    ))
    return out[:, :, :width] if padded != width else out


def solution(mesh):
    placed = (
        P("chain", None, "col"),
        P("chain", "col", None),
        P("chain", "col", None),
        P("chain", "col", None),
        P(None, "col"),
    )
    return jax.shard_map(
        functools.partial(shards, mesh.shape["chain"], mesh.shape["col"]),
        mesh=mesh, in_specs=placed, out_specs=P("chain", None, "col"), check_vma=False,
    )
```
